16 devices in a mesh: rep: 1, dp: 16 (over x, y, z, core).
Axes of the slice: x: 2, y: 2, z: 2, core: 2. Of those that a mesh axis runs over, the one named last changes fastest.
Arguments:
- x: bfloat16 [16, 2048, 640], P(('rep', 'dp'))
- dy: bfloat16 [16, 2048, 640], P(('rep', 'dp'))
- wq: bfloat16 [2, 640, 512], replicated
- wk: bfloat16 [2, 640, 128], replicated
- wv: bfloat16 [2, 640, 128], replicated
- wo: bfloat16 [2, 512, 640], replicated
- w_gate: bfloat16 [2, 640, 4096], replicated
- w_up: bfloat16 [2, 640, 4096], replicated
- w_down: bfloat16 [2, 4096, 640], replicated
- m_wq: float32 [2, 640, 512], P(None, 'dp')
- m_wk: float32 [2, 640, 128], P(None, 'dp')
- m_wv: float32 [2, 640, 128], P(None, 'dp')
- m_wo: float32 [2, 512, 640], P(None, 'dp')
- m_w_gate: float32 [2, 640, 4096], P(None, 'dp')
- m_w_up: float32 [2, 640, 4096], P(None, 'dp')
- m_w_down: float32 [2, 4096, 640], P(None, 'dp')
- v_wq: float32 [2, 640, 512], P(None, 'dp')
- v_wk: float32 [2, 640, 128], P(None, 'dp')
- v_wv: float32 [2, 640, 128], P(None, 'dp')
- v_wo: float32 [2, 512, 640], P(None, 'dp')
- v_w_gate: float32 [2, 640, 4096], P(None, 'dp')
- v_w_up: float32 [2, 640, 4096], P(None, 'dp')
- v_w_down: float32 [2, 4096, 640], P(None, 'dp')
Outputs:
- output 1: bfloat16 [2, 640, 512], P('rep')
- output 2: bfloat16 [2, 640, 128], P('rep')
- output 3: bfloat16 [2, 640, 128], P('rep')
- output 4: bfloat16 [2, 512, 640], P('rep')
- output 5: bfloat16 [2, 640, 4096], P('rep')
- output 6: bfloat16 [2, 640, 4096], P('rep')
- output 7: bfloat16 [2, 4096, 640], P('rep')
- output 8: float32 [2, 640, 512], P('rep', 'dp')
- output 9: float32 [2, 640, 128], P('rep', 'dp')
- output 10: float32 [2, 640, 128], P('rep', 'dp')
- output 11: float32 [2, 512, 640], P('rep', 'dp')
- output 12: float32 [2, 640, 4096], P('rep', 'dp')
- output 13: float32 [2, 640, 4096], P('rep', 'dp')
- output 14: float32 [2, 4096, 640], P('rep', 'dp')
- output 15: float32 [2, 640, 512], P('rep', 'dp')
- output 16: float32 [2, 640, 128], P('rep', 'dp')
- output 17: float32 [2, 640, 128], P('rep', 'dp')
- output 18: float32 [2, 512, 640], P('rep', 'dp')
- output 19: float32 [2, 640, 4096], P('rep', 'dp')
- output 20: float32 [2, 640, 4096], P('rep', 'dp')
- output 21: float32 [2, 4096, 640], P('rep', 'dp')
All inputs are finite; a program needn't handle non-finite values.
Results may differ from the reference program's by a relative error of at most 0.0258.
Values are sent between devices in bfloat16 or wider.
A program may use at most 2 GiB of HBM per device.

```python
import jax
import jax.numpy as jnp
from jax import lax

SEQUENCES = 16
TOKENS = 2048
D = 640
HEADS = 4
KV_HEADS = 1
HEAD = 128
FF = 4096
LAYERS = 2
THETA = 10000
NAMES = ("wq", "wk", "wv", "wo", "w_gate", "w_up", "w_down")
SHAPES = {
    "wq": (LAYERS, D, HEADS * HEAD),
    "wk": (LAYERS, D, KV_HEADS * HEAD),
    "wv": (LAYERS, D, KV_HEADS * HEAD),
    "wo": (LAYERS, HEADS * HEAD, D),
    "w_gate": (LAYERS, D, FF),
    "w_up": (LAYERS, D, FF),
    "w_down": (LAYERS, FF, D),
}


def bump(key, n, height):
    away = (jnp.arange(n, dtype=jnp.int32) - jax.random.randint(key, (), 0, n, jnp.int32)) % n
    return jnp.where(away < n // 8, height, 1.0)


def together(key, own, strength):
    shared = jax.random.normal(key, own.shape[1:], jnp.float32)
    return (own + strength * shared) * lax.rsqrt(1 + strength * strength)


def setup_inputs(seed: int = 0, part: int = 0) -> dict:
    kx, kdy, ka, kb, kz, kf, kh, kl, *keys = jax.random.split(jax.random.key(seed), 8 + 3 * len(NAMES))
    kx, kdy, ka, kb = (jax.random.fold_in(k, part) for k in (kx, kdy, ka, kb))
    kw, km, kv = (keys[i::3] for i in range(3))
    shape = (SEQUENCES, TOKENS, D)
    much_x, much_dy = jax.random.uniform(kz, (2,), jnp.float32, 0.0, 1.0)
    loud = 2.0 ** jax.random.uniform(jax.random.fold_in(kz, 1), (), jnp.float32, -1.0, 2.0)
    layers = 2.0 ** jax.random.uniform(kl, (LAYERS, 1, 1), jnp.float32, -1.0, 1.0)
    times = {"wq": 1.0, "wk": 1.0, "wv": 2.0, "wo": layers, "w_gate": 1.0, "w_up": bump(kh, FF, 4.0), "w_down": layers}
    x = together(ka, jax.random.normal(kx, shape, jnp.float32), much_x) * bump(kf, D, 4.0)
    dy = together(kb, jax.random.normal(kdy, shape, jnp.float32), much_dy)
    drawn = {"x": x.astype(jnp.bfloat16), "dy": (loud * dy * (SEQUENCES * TOKENS) ** -0.5).astype(jnp.bfloat16)}
    for key, name in zip(kw, NAMES, strict=True):
        drawn[name] = (jax.random.normal(key, SHAPES[name], jnp.float32) * SHAPES[name][1] ** -0.5 * times[name]).astype(jnp.bfloat16)
    for key, name in zip(km, NAMES, strict=True):
        drawn[f"m_{name}"] = 0.1 * jax.random.normal(key, SHAPES[name], jnp.float32)
    for key, name in zip(kv, NAMES, strict=True):
        drawn[f"v_{name}"] = jax.random.uniform(key, SHAPES[name], jnp.float32, 0.02, 0.06)
    return drawn


def matmul(a, w):
    return jnp.dot(a, w, preferred_element_type=jnp.float32).astype(jnp.bfloat16)


def normed(h):
    wide = h.astype(jnp.float32)
    scale = lax.rsqrt(jnp.mean(wide**2, -1, keepdims=True) + 1e-6)
    return (wide * scale).astype(jnp.bfloat16)


def turned(t, theta):
    half = t.shape[-1] // 2
    angle = jnp.arange(t.shape[0], dtype=jnp.float32)[:, None] * theta ** (-jnp.arange(half, dtype=jnp.float32) / half)
    cos, sin = jnp.cos(angle)[:, None], jnp.sin(angle)[:, None]
    a, b = t[..., :half].astype(jnp.float32), t[..., half:].astype(jnp.float32)
    return jnp.concatenate([a * cos - b * sin, b * cos + a * sin], -1).astype(jnp.bfloat16)


def seen_by(q, k, v):
    tokens, kv = q.shape[0], k.shape[1]
    q = q.reshape(tokens, kv, -1, q.shape[-1])
    scores = jnp.einsum("tgsd,ugd->gstu", q.astype(jnp.float32), k.astype(jnp.float32)) * q.shape[-1] ** -0.5
    place = jnp.arange(tokens)
    weights = jax.nn.softmax(jnp.where(place[:, None] >= place, scores, -jnp.inf), -1).astype(jnp.bfloat16)
    return jnp.einsum("gstu,ugd->tgsd", weights.astype(jnp.float32), v.astype(jnp.float32)).astype(jnp.bfloat16).reshape(tokens, -1)


def layer(h, w):
    a = normed(h)
    q, k = (turned(matmul(a, w[name]).reshape(h.shape[0], -1, HEAD), THETA) for name in ("wq", "wk"))
    h = h + matmul(seen_by(q, k, matmul(a, w["wv"]).reshape(h.shape[0], -1, HEAD)), w["wo"])
    b = normed(h)
    gate = jnp.dot(b, w["w_gate"], preferred_element_type=jnp.float32)
    up = jnp.dot(b, w["w_up"], preferred_element_type=jnp.float32)
    return h + matmul((jax.nn.silu(gate) * up).astype(jnp.bfloat16), w["w_down"])


def adamw(w, m, v, g):
    m = 0.9 * m + 0.1 * g
    v = 0.95 * v + 0.05 * g * g
    step = m * lax.rsqrt(v + 1e-8) + 0.1 * w
    return (w - 0.02 * step).astype(jnp.bfloat16), m, v


def clipped(gradients, sum_of_squares, count):
    factor = jnp.minimum(1.0, 0.5 * lax.rsqrt(sum_of_squares / count + 1e-30))
    return [g * factor for g in gradients]


def stack(weights, h):
    return lax.scan(lambda h, w: (layer(h, w), None), h, weights)[0]


def reference(x, dy, wq, wk, wv, wo, w_gate, w_up, w_down, m_wq, m_wk, m_wv, m_wo, m_w_gate, m_w_up, m_w_down, v_wq, v_wk, v_wv, v_wo, v_w_gate, v_w_up, v_w_down):
    weights = dict(zip(NAMES, (wq, wk, wv, wo, w_gate, w_up, w_down), strict=True))

    def take(so_far, sequence):
        h, by_y = sequence
        _, back = jax.vjp(stack, weights, h)
        by_weights, by_h = back(by_y)
        return jax.tree.map(lambda total, term: total + term.astype(jnp.float32), so_far, by_weights), by_h

    none_yet = {name: jnp.zeros(w.shape, jnp.float32) for name, w in weights.items()}
    by_weights, by_x = lax.scan(take, none_yet, (x, dy))
    gradients = [by_weights[name].astype(jnp.bfloat16).astype(jnp.float32) for name in NAMES]
    gradients = clipped(gradients, sum(jnp.sum(g * g) for g in gradients), sum(g.size for g in gradients))
    first = (m_wq, m_wk, m_wv, m_wo, m_w_gate, m_w_up, m_w_down)
    second = (v_wq, v_wk, v_wv, v_wo, v_w_gate, v_w_up, v_w_down)
    new = [adamw(weights[name].astype(jnp.float32), m, v, g) for name, m, v, g in zip(NAMES, first, second, gradients, strict=True)]
    return tuple(one[which] for which in range(3) for one in new)
```

```python
import functools

import jax
import jax.numpy as jnp
import numpy as np
from jax import lax
from jax.experimental import pallas as pl
from jax.experimental.pallas import tpu as pltpu
from jax.sharding import PartitionSpec as P

LOW = jnp.bfloat16
WIDE = jnp.float32
LOG2E = 1.4426950408889634
VMEM = 56 * 2**20
NEG = -1e30
HEAD = 128
SCALE = HEAD**-0.5
THETA = 10000


def _dot(a, b, ca=1, cb=0):
    return lax.dot_general(a, b, (((ca,), (cb,)), ((), ())), preferred_element_type=WIDE)


def _strips(q_ref, width):
    return [(n, at, at // width) for n in range(q_ref.shape[0]) for at in range(0, q_ref.shape[1], width)]


def _blocks(block, pieces, i, per):
    lax.fori_loop(0, i * per, lambda j, _: block(j, pieces, ()), None)
    for n in range(per):
        block(i * per + n, [p for p in pieces if p[2] >= n], [p for p in pieces if p[2] == n])


def _attend(q_ref, k_ref, v_ref, o_ref, lse_ref, top_s, mix_s, *, width):
    heads, bq, d = q_ref.shape
    pieces = _strips(q_ref, width)
    e = SCALE * LOG2E
    column = lambda p: pl.ds(p[0] * bq + p[1], width)
    top_s[...] = jnp.full(top_s.shape, NEG, WIDE)
    mix_s[...] = jnp.zeros(mix_s.shape, WIDE)
    ones = jnp.ones((8, width), LOW)

    def block(j, some, masked):
        here = pl.ds(pl.multiple_of(j * width, width), width)
        k = k_ref[here, :]
        values = jnp.concatenate([v_ref[here, :].T, ones], axis=0)
        scores = [_dot(k, q_ref[p[0], pl.ds(p[1], width), :], cb=1) for p in some]
        weights, keeps = [], []
        for p, s in zip(some, scores):
            if p in masked:
                s = jnp.where(lax.broadcasted_iota(jnp.int32, s.shape, 1) >= lax.broadcasted_iota(jnp.int32, s.shape, 0), s, 2 * NEG)
            old = top_s[:, column(p)]
            top = jnp.maximum(old, s.max(axis=0, keepdims=True))
            top_s[:, column(p)] = top
            weights.append(jnp.exp2((s - top) * e).astype(LOW))
            keeps.append(jnp.exp2((old - top) * e))
        for p, w, keep in zip(some, weights, keeps):
            mix_s[:, column(p)] = mix_s[:, column(p)] * keep + _dot(values, w)

    _blocks(block, pieces, pl.program_id(0), bq // width)
    for n in range(heads):
        cut = pl.ds(n * bq, bq)
        total = mix_s[d : d + 1, cut]
        o_ref[n] = (mix_s[:d, cut] * (1 / total)).T.astype(LOW)
        lse_ref[n : n + 1, :] = top_s[:, cut] * SCALE + jnp.log(total)


def attend(q, k, v, bq=1024, width=512):
    heads, t, d = q.shape
    block, whole = pl.BlockSpec((heads, bq, d), lambda i: (0, i, 0)), pl.BlockSpec((t, d), lambda i: (0, 0))
    return pl.pallas_call(
        functools.partial(_attend, width=width),
        grid=(t // bq,),
        in_specs=[block, whole, whole],
        out_specs=[block, pl.BlockSpec((heads, bq), lambda i: (0, i))],
        out_shape=[jax.ShapeDtypeStruct(q.shape, LOW), jax.ShapeDtypeStruct((heads, t), WIDE)],
        scratch_shapes=[pltpu.VMEM((1, heads * bq), WIDE), pltpu.VMEM((d + 8, heads * bq), WIDE)],
        compiler_params=pltpu.CompilerParams(dimension_semantics=("arbitrary",), vmem_limit_bytes=VMEM),
        cost_estimate=pl.CostEstimate(flops=4 * heads * t * t * d, transcendentals=heads * t * t, bytes_accessed=6 * heads * t * d),
        name="attend",
    )(q, k, v)


def _attend_back(q_ref, k_ref, v_ref, do_ref, lse_ref, delta_ref, dq_ref, dk_ref, dv_ref, dq_s, dk_s, dv_s, *, width):
    heads, bq, d = q_ref.shape
    pieces = _strips(q_ref, width)
    i = pl.program_id(0)

    @pl.when(i == 0)
    def _():
        dk_s[...] = jnp.zeros_like(dk_s)
        dv_s[...] = jnp.zeros_like(dv_s)

    dq_s[...] = jnp.zeros_like(dq_s)

    def block(j, some, masked):
        here = pl.ds(pl.multiple_of(j * width, width), width)
        k, v = k_ref[here, :], v_ref[here, :]
        kt = k.T
        qs = [q_ref[p[0], pl.ds(p[1], width), :] for p in some]
        dos = [do_ref[p[0], pl.ds(p[1], width), :] for p in some]
        scores = [_dot(k, x, cb=1) for x in qs]
        dps = [_dot(v, x, cb=1) for x in dos]
        for p, q, do, s, dp in zip(some, qs, dos, scores, dps):
            row = lambda ref: ref[p[0] : p[0] + 1, pl.ds(p[1], width)]
            w = jnp.exp2(s * (SCALE * LOG2E) - row(lse_ref) * LOG2E)
            if p in masked:
                w = jnp.where(lax.broadcasted_iota(jnp.int32, s.shape, 1) >= lax.broadcasted_iota(jnp.int32, s.shape, 0), w, 0.0)
            ds = (w * (dp - row(delta_ref))).astype(LOW)
            dv_s[here, :] += _dot(w.astype(LOW), do)
            dk_s[here, :] += _dot(ds, q)
            dq_s[:, pl.ds(p[0] * bq + p[1], width)] += _dot(kt, ds)

    _blocks(block, pieces, i, bq // width)
    for n in range(heads):
        dq_ref[n] = (dq_s[:, pl.ds(n * bq, bq)] * SCALE).T.astype(LOW)

    @pl.when(i == pl.num_programs(0) - 1)
    def _():
        dk_ref[...] = (dk_s[...] * SCALE).astype(LOW)
        dv_ref[...] = dv_s[...].astype(LOW)


def attend_back(q, k, v, do, lse, delta, bq=1024, width=256):
    heads, t, d = q.shape
    block, whole = pl.BlockSpec((heads, bq, d), lambda i: (0, i, 0)), pl.BlockSpec((t, d), lambda i: (0, 0))
    row = pl.BlockSpec((heads, bq), lambda i: (0, i))
    return pl.pallas_call(
        functools.partial(_attend_back, width=width),
        grid=(t // bq,),
        in_specs=[block, whole, whole, block, row, row],
        out_specs=[block, whole, whole],
        out_shape=[jax.ShapeDtypeStruct(a.shape, LOW) for a in (q, k, v)],
        scratch_shapes=[pltpu.VMEM((d, heads * bq), WIDE), pltpu.VMEM((t, d), WIDE), pltpu.VMEM((t, d), WIDE)],
        compiler_params=pltpu.CompilerParams(dimension_semantics=("arbitrary",), vmem_limit_bytes=VMEM),
        cost_estimate=pl.CostEstimate(flops=10 * heads * t * t * d, transcendentals=heads * t * t, bytes_accessed=9 * heads * t * d),
        name="attend_back",
    )(q, k, v, do, lse, delta)


AXES = (8, 4, 2)
ORDERS = ((0, 1, 2), (1, 2, 0), (2, 0, 1))


def normed(h):
    wide = h.astype(jnp.float32)
    scale = lax.rsqrt(jnp.mean(wide**2, -1, keepdims=True) + 1e-6)
    return (wide * scale).astype(jnp.bfloat16)


def by_normed(h, by_b):
    h, by_b = h.astype(WIDE), by_b.astype(LOW).astype(WIDE)
    scale = lax.rsqrt(jnp.mean(h * h, -1, keepdims=True) + 1e-6)
    return by_b * scale - h * (scale * scale * scale * jnp.mean(by_b * h, -1, keepdims=True))


def angles(tokens):
    half = HEAD // 2
    angle = np.arange(tokens, dtype=np.float32)[:, None] * np.float32(THETA) ** (-np.arange(half, dtype=np.float32) / np.float32(half))
    return jnp.asarray(np.concatenate([np.cos(angle), np.sin(angle)], -1).astype(np.float32))


def _cos_sin(table):
    half = HEAD // 2
    other = pltpu.roll(table, half, 1)
    first = lax.broadcasted_iota(jnp.int32, table.shape, 1) < half
    return jnp.where(first, table, other), jnp.where(first, -other, table)


def _turn(t, cos, sin):
    wide = t.astype(WIDE)
    return (wide * cos + pltpu.roll(wide, HEAD // 2, 1) * sin).astype(LOW)


def _before(h_ref, turn_ref, wq_ref, wk_ref, wv_ref, q_ref, k_ref, v_ref):
    a = normed(h_ref[...])
    cos, sin = _cos_sin(turn_ref[...])
    q = _dot(a, wq_ref[...]).astype(LOW)
    for n in range(q_ref.shape[0]):
        q_ref[n] = _turn(q[:, n * HEAD : (n + 1) * HEAD], cos, sin)
    kv = _dot(a, jnp.concatenate([wk_ref[...], wv_ref[...]], 1)).astype(LOW)
    k_ref[...] = _turn(kv[:, :HEAD], cos, sin)
    v_ref[...] = kv[:, HEAD:]


def _of_layer(number, w):
    return pl.BlockSpec((None, *w.shape[1:]), lambda *_: (number, 0, 0))


def before(number, h, turns, wq, wk, wv, tb=512):
    t, d = h.shape
    heads = wq.shape[2] // HEAD
    row = lambda i: (i, 0)
    return pl.pallas_call(
        _before,
        grid=(t // tb,),
        in_specs=[pl.BlockSpec((tb, d), row), pl.BlockSpec((tb, HEAD), row), *(_of_layer(number, w) for w in (wq, wk, wv))],
        out_specs=[pl.BlockSpec((heads, tb, HEAD), lambda i: (0, i, 0)), pl.BlockSpec((tb, HEAD), row), pl.BlockSpec((tb, HEAD), row)],
        out_shape=[jax.ShapeDtypeStruct((heads, t, HEAD), LOW), jax.ShapeDtypeStruct((t, HEAD), LOW), jax.ShapeDtypeStruct((t, HEAD), LOW)],
        compiler_params=pltpu.CompilerParams(dimension_semantics=("arbitrary",), vmem_limit_bytes=VMEM),
        cost_estimate=pl.CostEstimate(flops=2 * t * d * (heads + 2) * HEAD, transcendentals=t, bytes_accessed=4 * t * d),
        name="before",
    )(h, turns, wq, wk, wv)


def _halve(core, acc_s, refs):
    if len(refs) == 1:
        refs[0][...] = acc_s[...].astype(LOW)
        return
    rows = refs[0].shape[1]
    for n in range(8):
        for to, at in zip(refs, (core, 1 - core)):
            to[n] = acc_s[pl.ds(pl.multiple_of((2 * n + at) * rows, 8), rows), :].astype(LOW)


def _gradient(rows, columns, halves):
    return [jax.ShapeDtypeStruct((8, rows // 16, columns), LOW)] * 2 if halves else [jax.ShapeDtypeStruct((rows, columns), LOW)]


def _at_start(shapes):
    return [pl.BlockSpec(one.shape, lambda i, n=len(one.shape): (0,) * n) for one in shapes]


def _after_back(core_ref, dmid_ref, att_ref, wo_ref, datt_ref, delta_ref, *rest):
    *out_refs, acc_s = rest
    i = pl.program_id(0)
    dmid = dmid_ref[...]
    heads = att_ref.shape[0]
    datt = _dot(dmid, wo_ref[...], cb=1).astype(LOW)
    for n in range(heads):
        one = datt[:, n * HEAD : (n + 1) * HEAD]
        datt_ref[n] = one
        delta_ref[n : n + 1, :] = (one.astype(WIDE) * att_ref[n].astype(WIDE)).T.sum(0, keepdims=True)
    term = jnp.concatenate([_dot(att_ref[n].T, dmid) for n in range(heads)], 0)

    @pl.when(i == 0)
    def _():
        acc_s[...] = term

    @pl.when(i > 0)
    def _():
        acc_s[...] += term

    @pl.when(i == pl.num_programs(0) - 1)
    def _():
        _halve(core_ref[0], acc_s, out_refs)


def after_back(number, core, dmid, att, wo, halves, tb=512):
    t, d = dmid.shape
    heads = att.shape[0]
    head = pl.BlockSpec((heads, tb, HEAD), lambda i: (0, i, 0))
    grad = _gradient(heads * HEAD, d, halves)
    return pl.pallas_call(
        _after_back,
        grid=(t // tb,),
        in_specs=[pl.BlockSpec(memory_space=pltpu.SMEM), pl.BlockSpec((tb, d), lambda i: (i, 0)), head, _of_layer(number, wo)],
        out_specs=[head, pl.BlockSpec((heads, tb), lambda i: (0, i)), *_at_start(grad)],
        out_shape=[jax.ShapeDtypeStruct(att.shape, LOW), jax.ShapeDtypeStruct((heads, t), WIDE), *grad],
        scratch_shapes=[pltpu.VMEM((heads * HEAD, d), WIDE)],
        compiler_params=pltpu.CompilerParams(dimension_semantics=("arbitrary",), vmem_limit_bytes=VMEM),
        cost_estimate=pl.CostEstimate(flops=4 * t * d * heads * HEAD, transcendentals=0, bytes_accessed=8 * t * d),
        name="after_back",
    )(core, dmid, att, wo)


def _before_back(core_ref, h_ref, turn_ref, dq_ref, dk_ref, dv_ref, *rest, inner):
    if inner:
        dmid_ref, wq_ref, wk_ref, wv_ref, dh_ref, *rest = rest
    *out_refs, acc_s = rest
    i = pl.program_id(0)
    cos, sin = _cos_sin(turn_ref[...])
    sin = -sin
    by = jnp.concatenate([_turn(dq_ref[n], cos, sin) for n in range(dq_ref.shape[0])] + [_turn(dk_ref[...], cos, sin), dv_ref[...]], 1)
    term = _dot(normed(h_ref[...]).T, by)

    @pl.when(i == 0)
    def _():
        acc_s[...] = term

    @pl.when(i > 0)
    def _():
        acc_s[...] += term

    if inner:
        w = jnp.concatenate([wq_ref[...], wk_ref[...], wv_ref[...]], 1)
        dh_ref[...] = (dmid_ref[...].astype(WIDE) + by_normed(h_ref[...], _dot(by, w, cb=1))).astype(LOW)

    @pl.when(i == pl.num_programs(0) - 1)
    def _():
        _halve(core_ref[0], acc_s, out_refs)


def before_back(number, core, h, turns, dq, dk, dv, dmid, wq, wk, wv, inner, halves, tb=512):
    t, d = h.shape
    heads = dq.shape[0]
    wide = (heads + 2) * HEAD
    row = lambda i: (i, 0)
    states, head = pl.BlockSpec((tb, d), row), pl.BlockSpec((tb, HEAD), row)
    grad = _gradient(d, wide, halves)
    more = [states, *(_of_layer(number, w) for w in (wq, wk, wv))] if inner else []
    return pl.pallas_call(
        functools.partial(_before_back, inner=inner),
        grid=(t // tb,),
        in_specs=[pl.BlockSpec(memory_space=pltpu.SMEM), states, head, pl.BlockSpec((heads, tb, HEAD), lambda i: (0, i, 0)), head, head, *more],
        out_specs=([states] if inner else []) + _at_start(grad),
        out_shape=([jax.ShapeDtypeStruct((t, d), LOW)] if inner else []) + grad,
        scratch_shapes=[pltpu.VMEM((d, wide), WIDE)],
        compiler_params=pltpu.CompilerParams(dimension_semantics=("arbitrary",), vmem_limit_bytes=VMEM),
        cost_estimate=pl.CostEstimate(flops=(4 if inner else 2) * t * d * wide, transcendentals=t, bytes_accessed=10 * t * d),
        name="before_back",
    )(core, h, turns, dq, dk, dv, *([dmid, wq, wk, wv] if inner else []))


def _mlp_forward(h_ref, att_ref, wo_ref, wg_ref, wu_ref, wd_ref, mid_ref, y_ref, gate_ref, up_ref, b_s, mid_s, acc_s, *, tb, strip):
    j, i = pl.program_id(0), pl.program_id(1)
    last = pl.num_programs(0) - 1
    for at in range(0, tb, strip):
        here = pl.ds(pl.multiple_of(i * tb + at, strip), strip)
        cut = pl.ds(at, strip)

        @pl.when(j == 0)
        def _():
            mid = (h_ref[cut, :].astype(WIDE) + _dot(jnp.concatenate([att_ref[n, cut, :] for n in range(att_ref.shape[0])], 1), wo_ref[...]).astype(LOW).astype(WIDE)).astype(LOW)
            mid_ref[cut, :] = mid
            mid_s[here, :] = mid
            b_s[here, :] = normed(mid)
            acc_s[here, :] = jnp.zeros((strip, acc_s.shape[1]), WIDE)

    here = [pl.ds(pl.multiple_of(i * tb + at, strip), strip) for at in range(0, tb, strip)]
    both = lambda n: [_dot(b_s[here[n], :], w[...]) for w in (wg_ref, wu_ref)]
    ahead = both(0)
    for n in range(len(here)):
        gate, up = ahead
        ahead = both(n + 1) if n + 1 < len(here) else None
        cut = pl.ds(n * strip, strip)
        gate_ref[cut, :] = gate
        up_ref[cut, :] = up
        t = (gate * (0.5 * jnp.tanh(0.5 * gate) + 0.5) * up).astype(LOW)
        acc_s[here[n], :] += _dot(t, wd_ref[...])

    @pl.when(j == last)
    def _():
        here = pl.ds(pl.multiple_of(i * tb, tb), tb)
        y_ref[...] = (mid_s[here, :].astype(WIDE) + acc_s[here, :].astype(LOW).astype(WIDE)).astype(LOW)


def _of_mlp(number, d, fb):
    side = pl.BlockSpec((None, d, fb), lambda j, i: (number, 0, j))
    return side, side, pl.BlockSpec((None, fb, d), lambda j, i: (number, j, 0))


def mlp_forward(number, h, att, wo, wg, wu, wd, tb=1024, fb=512, strip=256):
    t, d = h.shape
    ff, hd = wg.shape[2], wo.shape[1]
    n = t // tb
    at_first = lambda j, i: (jnp.where(j == 0, i, n - 1), 0)
    at_last = lambda j, i: (jnp.where(j == ff // fb - 1, i, 0), 0)
    return pl.pallas_call(
        functools.partial(_mlp_forward, tb=tb, strip=strip),
        grid=(ff // fb, n),
        in_specs=[pl.BlockSpec((tb, d), at_first), pl.BlockSpec((att.shape[0], tb, HEAD), lambda j, i: (0, at_first(j, i)[0], 0)), _of_layer(number, wo),
                  *_of_mlp(number, d, fb)],
        out_specs=[pl.BlockSpec((tb, d), at_first), pl.BlockSpec((tb, d), at_last),
                   *[pl.BlockSpec((tb, fb), lambda j, i: (i, j))] * 2],
        scratch_shapes=[pltpu.VMEM((t, d), LOW), pltpu.VMEM((t, d), LOW), pltpu.VMEM((t, d), WIDE)],
        out_shape=[jax.ShapeDtypeStruct((t, d), LOW), jax.ShapeDtypeStruct((t, d), LOW), jax.ShapeDtypeStruct((t, ff), WIDE),
                   jax.ShapeDtypeStruct((t, ff), WIDE)],
        compiler_params=pltpu.CompilerParams(dimension_semantics=("arbitrary", "arbitrary"), vmem_limit_bytes=VMEM),
        cost_estimate=pl.CostEstimate(flops=2 * t * d * (3 * ff + hd), transcendentals=t * ff, bytes_accessed=8 * t * ff + 6 * d * ff + 10 * t * d),
        name="mlp_forward",
    )(h, att, wo, wg, wu, wd)


def _mlp_backward(core_ref, dy_ref, mid_ref, gate_ref, up_ref, wg_ref, wu_ref, wd_ref, dmid_ref, *rest, tb, strip):
    *out_refs, bt_s, dyt_s, db_s, pg_s, pu_s, t_s, ag_s, au_s, ad_s = rest
    per = len(out_refs) // 3
    j, i = pl.program_id(0), pl.program_id(1)
    all_i = pl.ds(pl.multiple_of(i * tb, tb), tb)

    @pl.when(j == 0)
    def _():
        for at in range(0, tb, strip):
            here = pl.ds(pl.multiple_of(i * tb + at, strip), strip)
            bt_s[:, here] = normed(mid_ref[here, :]).T
            dyt_s[:, here] = dy_ref[here, :].T
            db_s[here, :] = jnp.zeros((strip, db_s.shape[1]), WIDE)

    @pl.when(i == 0)
    def _():
        for ref in (ag_s, au_s, ad_s):
            ref[...] = jnp.zeros_like(ref)

    for at in range(0, tb, strip):
        here = pl.ds(pl.multiple_of(i * tb + at, strip), strip)
        cut = pl.ds(at, strip)
        dt = _dot(dy_ref[here, :], wd_ref[...], cb=1).astype(LOW).astype(WIDE)
        gate, up = gate_ref[cut, :], up_ref[cut, :]
        half = 0.5 * jnp.tanh(0.5 * gate)
        sig = half + 0.5
        silu = gate * sig
        by_up = (dt * silu).astype(LOW)
        by_gate = (dt * up * (sig + silu * (0.5 - half))).astype(LOW)
        t_s[cut, :] = (silu * up).astype(LOW)
        pg_s[cut, :] = by_gate
        pu_s[cut, :] = by_up
        db_s[here, :] += _dot(by_gate, wg_ref[...], cb=1) + _dot(by_up, wu_ref[...], cb=1)

    ag_s[...] += _dot(bt_s[:, all_i], pg_s[...])
    au_s[...] += _dot(bt_s[:, all_i], pu_s[...])
    ad_s[...] += _dot(dyt_s[:, all_i], t_s[...])

    @pl.when(i == pl.num_programs(1) - 1)
    def _():
        core = core_ref[0]
        _halve(core, ag_s, out_refs[:per])
        _halve(core, au_s, out_refs[per : 2 * per])
        down = out_refs[2 * per :]
        if per == 1:
            down[0][...] = ad_s[...].T.astype(LOW)
        else:
            wide = down[0].shape[1]
            for to, at in zip(down, (core, 1 - core)):
                to[0] = ad_s[:, pl.ds(pl.multiple_of(at * wide, 128), wide)].T.astype(LOW)

    @pl.when(j == pl.num_programs(0) - 1)
    def _():
        for at in range(0, tb, strip):
            here = pl.ds(pl.multiple_of(i * tb + at, strip), strip)
            cut = pl.ds(at, strip)
            dmid_ref[cut, :] = (dy_ref[here, :].astype(WIDE) + by_normed(mid_ref[here, :], db_s[here, :])).astype(LOW)


def mlp_backward(number, core, dy, mid, gate, up, wg, wu, wd, halves, tb=1024, strip=256):
    t, d = dy.shape
    ff = wg.shape[2]
    n, fb = t // tb, ff // 8
    whole = lambda j, i: (0, 0)
    at_last = lambda j, i: (jnp.where(j == 7, i, 0), 0)
    rows = d // 16
    if halves:
        side, tall = [pl.BlockSpec((8, rows, fb), lambda j, i: (0, 0, j))] * 2, [pl.BlockSpec((1, fb // 2, d), lambda j, i: (j, 0, 0))] * 2
    else:
        side, tall = [pl.BlockSpec((d, fb), lambda j, i: (0, j))], [pl.BlockSpec((fb, d), lambda j, i: (j, 0))]
    one = pl.Buffered(1)
    return pl.pallas_call(
        functools.partial(_mlp_backward, tb=tb, strip=strip),
        grid=(8, n),
        in_specs=[pl.BlockSpec(memory_space=pltpu.SMEM), pl.BlockSpec((t, d), whole, pipeline_mode=one), pl.BlockSpec((t, d), whole, pipeline_mode=one),
                  *[pl.BlockSpec((tb, fb), lambda j, i: (i, j))] * 2,
                  *_of_mlp(number, d, fb)],
        out_specs=[pl.BlockSpec((tb, d), at_last), *side, *side, *tall],
        scratch_shapes=[pltpu.VMEM((d, t), LOW), pltpu.VMEM((d, t), LOW), pltpu.VMEM((t, d), WIDE)] + [pltpu.VMEM((tb, fb), LOW)] * 3
        + [pltpu.VMEM((d, fb), WIDE)] * 3,
        out_shape=[jax.ShapeDtypeStruct((t, d), LOW), *_gradient(d, ff, halves), *_gradient(d, ff, halves), *_gradient(ff, d, halves)],
        compiler_params=pltpu.CompilerParams(dimension_semantics=("arbitrary", "arbitrary"), vmem_limit_bytes=VMEM),
        cost_estimate=pl.CostEstimate(flops=12 * t * d * ff, transcendentals=t * ff, bytes_accessed=8 * t * ff + 12 * d * ff + 6 * t * d),
        name="mlp_backward",
    )(core, dy, mid, gate, up, wg, wu, wd)


def swapped(t, step):
    return lax.ppermute(t, "dp", [(n, n ^ step) for n in range(16)])


class Reduction:
    def __init__(self, place, pairs, orders):
        self.place, self.orders, self.at = place, orders, 0
        self.held = [[keep.reshape(2, 2, 2, *keep.shape[1:])] for keep, _ in pairs]
        self.out = [send for _, send in pairs]

    def go(self):
        self.got = [swapped(t, AXES[order[self.at - 1]] if self.at else 1) for t, order in zip(self.out, self.orders)]

    def take(self):
        total = lambda parts: functools.reduce(jnp.add, [p.astype(WIDE) for p in parts]).astype(LOW)
        for n, order in enumerate(self.orders):
            self.held[n].append(self.got[n].reshape(self.held[n][0].shape))
            if self.at == 3:
                self.out[n] = total(self.held[n]).reshape(self.held[n][0].shape[3:]).astype(WIDE)
                continue
            axis = order[self.at]
            mine = self.place // AXES[axis] % 2
            pick = lambda t, at: lax.dynamic_index_in_dim(t, at, axis, keepdims=True)
            self.out[n] = total([pick(t, 1 - mine) for t in self.held[n]])
            self.held[n] = [pick(t, mine) for t in self.held[n]]
        self.at += 1


def landed(x, *reductions):
    x, got = lax.optimization_barrier((x, [r.got for r in reductions]))
    for r, new in zip(reductions, got):
        r.got = new
        r.take()
    x, out = lax.optimization_barrier((x, [r.out for r in reductions]))
    for r, new in zip(reductions, out):
        r.out = new
        if r.at < 4:
            r.go()
    return x


MESH_ID = pl.DeviceIdType.MESH


def _shared(x_ref, o_ref, all_s, send_sem, recv_sem):
    me = lax.axis_index("dp")
    barrier = pltpu.get_barrier_semaphore()
    for n in range(1, 16):
        pl.semaphore_signal(barrier, inc=1, device_id={"dp": (me + n) % 16}, device_id_type=MESH_ID)
    pl.semaphore_wait(barrier, 15)
    copies = [pltpu.make_async_remote_copy(src_ref=x_ref, dst_ref=all_s.at[n], send_sem=send_sem.at[n], recv_sem=recv_sem.at[n],
                                           device_id={"dp": (me + n) % 16}, device_id_type=MESH_ID) for n in range(1, 16)]
    for copy in copies:
        copy.start()
    total = x_ref[...]
    for copy in copies:
        copy.wait()
    for n in range(1, 16):
        total += all_s[n]
    o_ref[...] = total


def shared(x):
    return pl.pallas_call(
        _shared,
        in_specs=[pl.BlockSpec(memory_space=pltpu.VMEM)],
        out_specs=pl.BlockSpec(memory_space=pltpu.VMEM),
        out_shape=jax.ShapeDtypeStruct(x.shape, WIDE),
        scratch_shapes=[pltpu.VMEM((16, *x.shape), WIDE), pltpu.SemaphoreType.DMA((16,)), pltpu.SemaphoreType.DMA((16,))],
        compiler_params=pltpu.CompilerParams(collective_id=0, has_side_effects=True),
        name="shared",
    )(x)


def _gathered(*refs, turns):
    n = len(turns)
    ins, outs = refs[:n], refs[n : 2 * n]
    ici_send, ici_recv, pair_send, pair_recv, own_sem = refs[2 * n :]
    me = lax.axis_index("dp")
    steps = [s * (1 - 2 * (me // s % 2)) for s in AXES]
    other = 1 - 2 * (me % 2)
    barrier = pltpu.get_barrier_semaphore()
    for step in (*steps, other):
        pl.semaphore_signal(barrier, inc=1, device_id={"dp": me + step}, device_id_type=MESH_ID)
    pl.semaphore_wait(barrier, 4)

    def block(mask):
        return me + sum(steps[a] for a in range(3) if mask >> a & 1)

    def copy(k, mask, to, sems, row):
        src = ins[k] if mask == 0 else outs[k].at[:, block(mask)]
        return pltpu.make_async_remote_copy(src_ref=src, dst_ref=outs[k].at[:, block(mask)], send_sem=sems[0].at[k, row], recv_sem=sems[1].at[k, row],
                                            device_id={"dp": me + to}, device_id_type=MESH_ID)

    started = []

    def go(k, mask):
        order = ORDERS[turns[k]]
        last = max([order.index(a) for a in range(3) if mask >> a & 1], default=-1)
        for a in order[last + 1 :]:
            one = copy(k, mask, steps[a], (ici_send, ici_recv), mask | 1 << a)
            one.start()
            started.append(one)
        one = copy(k, mask, other, (pair_send, pair_recv), mask)
        one.start()
        started.append(one)

    def here(k, mask):
        copy(k, mask, steps[0], (ici_send, ici_recv), mask).wait_recv()
        go(k, mask)

    mine = [pltpu.make_async_copy(ins[k], outs[k].at[:, me], own_sem.at[k]) for k in range(n)]
    for k in range(n):
        go(k, 0)
    for one in mine:
        one.start()
    bit = lambda k, *at: sum(1 << ORDERS[turns[k]][a] for a in at)
    for sets in (((0,), (1,), (2,)), ((0, 1), (0, 2), (1, 2)), ((0, 1, 2),)):
        for k in range(n):
            for at in sets:
                here(k, bit(k, *at))
    for k in range(n):
        for mask in range(8):
            copy(k, mask, other, (pair_send, pair_recv), mask).wait_recv()
    for one in started:
        one.wait_send()
    for one in mine:
        one.wait()


def gathered(blocks, turns):
    hbm = pl.BlockSpec(memory_space=pl.ANY)
    n = len(blocks)
    sems = [pltpu.SemaphoreType.DMA((n, 8))] * 4 + [pltpu.SemaphoreType.DMA((n,))]
    return pl.pallas_call(
        functools.partial(_gathered, turns=turns),
        in_specs=[hbm] * n,
        out_specs=[hbm] * n,
        out_shape=[jax.ShapeDtypeStruct((b.shape[0], 16, *b.shape[1:]), b.dtype) for b in blocks],
        scratch_shapes=sems,
        compiler_params=pltpu.CompilerParams(collective_id=1, has_side_effects=True, vmem_limit_bytes=2**20),
        name="gathered",
    )(*blocks)


def _settled(*refs):
    n = len(refs) // 2
    copies = [pltpu.make_async_copy(refs[k], refs[n + k], refs[-1].at[k]) for k in range(n)]
    for copy in copies:
        copy.start()
    for copy in copies:
        copy.wait()


def settled(arrays):
    hbm = pl.BlockSpec(memory_space=pl.ANY)
    n = len(arrays)
    return pl.pallas_call(
        _settled,
        in_specs=[hbm] * n,
        out_specs=[hbm] * n,
        out_shape=[jax.ShapeDtypeStruct(a.shape, a.dtype) for a in arrays],
        scratch_shapes=[pltpu.SemaphoreType.DMA((n,))],
        compiler_params=pltpu.CompilerParams(vmem_limit_bytes=2**20),
        name="settled",
    )(*arrays)


def adamw(w, m, v, g):
    m = 0.9 * m + 0.1 * g
    v = 0.95 * v + 0.05 * g * g
    step = m * lax.rsqrt(v + 1e-8) + 0.1 * w
    return (w - 0.02 * step).astype(jnp.bfloat16), m, v


def clipped(gradients, sum_of_squares, count):
    factor = jnp.minimum(1.0, 0.5 * lax.rsqrt(sum_of_squares / count + 1e-30))
    return [g * factor for g in gradients]


def solution(mesh):
    def step(x, dy, *arrays):
        weights, m, v = (arrays[i : i + 7] for i in (0, 7, 14))
        layers = weights[0].shape[0]
        me = lax.axis_index("dp")
        core = (me % 2).astype(jnp.int32).reshape(1)
        wq, wk, wv, wo, wg, wu, wd = weights
        turns = angles(x.shape[1])
        h, kept = x[0], []
        for number in range(layers):
            q, k, val = before(number, h, turns, wq, wk, wv)
            att, lse = attend(q, k, val)
            mid, y, gate, up = mlp_forward(number, h, att, wo, wg, wu, wd)
            kept.append((h, q, k, val, att, lse, mid, gate, up))
            h = y
        by_h, mine = dy[0], [None] * layers
        scattered = lambda t: lax.psum_scatter(t, "dp", scatter_dimension=0, tiled=True).astype(WIDE)
        dq, dk = wq.shape[2], wk.shape[2]
        late_mlp, late_small = [], []
        for number in reversed(range(layers)):
            h, q, k, val, att, lse, mid, gate, up = kept[number]
            last = number == 0
            by_mid, *by_mlp = mlp_backward(number, core, by_h, mid, gate, up, wg, wu, wd, last)
            if last:
                big = Reduction(me, [by_mlp[n : n + 2] for n in (0, 2, 4)], ORDERS)
                big.go()
                by_mid, late_small, sides = lax.optimization_barrier((by_mid, late_small, [m[:2] for m in late_mlp]))
                late_small = [[scattered(t) for t in some] for some in late_small]
            by_att, delta, *by_o = after_back(number, core, by_mid, att, wo, last)
            if last:
                by_att, downs = lax.optimization_barrier((landed(by_att, big), [m[2] for m in late_mlp]))
            by_q, by_k, by_v = attend_back(q, k, val, by_att, lse, delta)
            if last:
                by_q, by_o = lax.optimization_barrier((landed(by_q, big), by_o))
            outs = before_back(number, core, h, turns, by_q, by_k, by_v, by_mid, wq, wk, wv, not last, last)
            if not last:
                by_h, by_qkv = outs
                late_mlp.append([scattered(t) for t in by_mlp])
                late_small.append([by_o[0], by_qkv])
        small = Reduction(me, [by_o, outs], ORDERS[:2])
        small.go()
        for r in (big, small):
            while r.at < 4:
                r.take()
                if r.at < 4:
                    r.go()
        mine = [[*small.out, *big.out]] + [[*some, *side, down] for some, side, down in zip(late_small, sides, downs)][::-1]
        mine = [[qkv[:, :dq], qkv[:, dq : dq + dk], qkv[:, dq + dk :], o, *mlp] for o, qkv, *mlp in mine]
        gradients = [jnp.stack([mine[number][i] for number in range(layers)]) for i in range(7)]
        local = sum(jnp.sum(g * g) for g in gradients)
        squares = shared(jnp.full((8, 128), local, WIDE))[0, 0]
        gradients = clipped(gradients, squares, 16 * sum(g.size for g in gradients))
        own = [lax.dynamic_slice_in_dim(w, me * one.shape[1], one.shape[1], 1).astype(jnp.float32) for w, one in zip(weights, m, strict=True)]
        new = [adamw(w, m, v, g) for w, m, v, g in zip(own, m, v, gradients, strict=True)]
        whole = gathered([one[0] for one in new], (0, 1, 1, 2, 0, 1, 2))
        whole = [t.reshape(t.shape[0], -1, t.shape[3]) for t in settled(whole)]
        return (*whole, *(one[1] for one in new), *(one[2] for one in new))

    states, all_of, cut = P(("rep", "dp"), None, None), P(None, None, None), P(None, "dp", None)
    return jax.shard_map(
        step,
        mesh=mesh,
        in_specs=(states, states) + (all_of,) * 7 + (cut,) * 14,
        out_specs=(P("rep", None, None),) * 7 + (P("rep", "dp", None),) * 14,
        check_vma=False,
    )
```

```python
import functools

import jax
import jax.numpy as jnp
import numpy as np
from jax import lax
from jax.experimental import pallas as pl
from jax.experimental.pallas import tpu as pltpu
from jax.sharding import PartitionSpec as P

LOW = jnp.bfloat16
WIDE = jnp.float32
LOG2E = 1.4426950408889634
VMEM = 56 * 2**20
NEG = -1e30
HEAD = 128
SCALE = HEAD**-0.5
THETA = 10000


def _dot(a, b, ca=1, cb=0):
    return lax.dot_general(a, b, (((ca,), (cb,)), ((), ())), preferred_element_type=WIDE)


def _strips(q_ref, width):
    return [(n, at, at // width) for n in range(q_ref.shape[0]) for at in range(0, q_ref.shape[1], width)]


def _blocks(block, pieces, i, per):
    lax.fori_loop(0, i * per, lambda j, _: block(j, pieces, ()), None)
    for n in range(per):
        block(i * per + n, [p for p in pieces if p[2] >= n], [p for p in pieces if p[2] == n])


def _attend(q_ref, k_ref, v_ref, o_ref, lse_ref, top_s, mix_s, *, width):
    heads, bq, d = q_ref.shape
    pieces = _strips(q_ref, width)
    e = SCALE * LOG2E
    column = lambda p: pl.ds(p[0] * bq + p[1], width)
    top_s[...] = jnp.full(top_s.shape, NEG, WIDE)
    mix_s[...] = jnp.zeros(mix_s.shape, WIDE)
    ones = jnp.ones((8, width), LOW)

    def block(j, some, masked):
        here = pl.ds(pl.multiple_of(j * width, width), width)
        k = k_ref[here, :]
        values = jnp.concatenate([v_ref[here, :].T, ones], axis=0)
        scores = [_dot(k, q_ref[p[0], pl.ds(p[1], width), :], cb=1) for p in some]
        weights, keeps = [], []
        for p, s in zip(some, scores):
            if p in masked:
                s = jnp.where(lax.broadcasted_iota(jnp.int32, s.shape, 1) >= lax.broadcasted_iota(jnp.int32, s.shape, 0), s, 2 * NEG)
            old = top_s[:, column(p)]
            top = jnp.maximum(old, s.max(axis=0, keepdims=True))
            top_s[:, column(p)] = top
            weights.append(jnp.exp2((s - top) * e).astype(LOW))
            keeps.append(jnp.exp2((old - top) * e))
        for p, w, keep in zip(some, weights, keeps):
            mix_s[:, column(p)] = mix_s[:, column(p)] * keep + _dot(values, w)

    _blocks(block, pieces, pl.program_id(0), bq // width)
    for n in range(heads):
        cut = pl.ds(n * bq, bq)
        total = mix_s[d : d + 1, cut]
        o_ref[n] = (mix_s[:d, cut] * (1 / total)).T.astype(LOW)
        lse_ref[n : n + 1, :] = top_s[:, cut] * SCALE + jnp.log(total)


def attend(q, k, v, bq=1024, width=512):
    heads, t, d = q.shape
    block, whole = pl.BlockSpec((heads, bq, d), lambda i: (0, i, 0)), pl.BlockSpec((t, d), lambda i: (0, 0))
    return pl.pallas_call(
        functools.partial(_attend, width=width),
        grid=(t // bq,),
        in_specs=[block, whole, whole],
        out_specs=[block, pl.BlockSpec((heads, bq), lambda i: (0, i))],
        out_shape=[jax.ShapeDtypeStruct(q.shape, LOW), jax.ShapeDtypeStruct((heads, t), WIDE)],
        scratch_shapes=[pltpu.VMEM((1, heads * bq), WIDE), pltpu.VMEM((d + 8, heads * bq), WIDE)],
        compiler_params=pltpu.CompilerParams(dimension_semantics=("arbitrary",), vmem_limit_bytes=VMEM),
        cost_estimate=pl.CostEstimate(flops=4 * heads * t * t * d, transcendentals=heads * t * t, bytes_accessed=6 * heads * t * d),
        name="attend",
    )(q, k, v)


def _attend_back(q_ref, k_ref, v_ref, do_ref, lse_ref, delta_ref, dq_ref, dk_ref, dv_ref, dq_s, dk_s, dv_s, *, width):
    heads, bq, d = q_ref.shape
    pieces = _strips(q_ref, width)
    i = pl.program_id(0)

    @pl.when(i == 0)
    def _():
        dk_s[...] = jnp.zeros_like(dk_s)
        dv_s[...] = jnp.zeros_like(dv_s)

    dq_s[...] = jnp.zeros_like(dq_s)

    def block(j, some, masked):
        here = pl.ds(pl.multiple_of(j * width, width), width)
        k, v = k_ref[here, :], v_ref[here, :]
        kt = k.T
        qs = [q_ref[p[0], pl.ds(p[1], width), :] for p in some]
        dos = [do_ref[p[0], pl.ds(p[1], width), :] for p in some]
        scores = [_dot(k, x, cb=1) for x in qs]
        dps = [_dot(v, x, cb=1) for x in dos]
        for p, q, do, s, dp in zip(some, qs, dos, scores, dps):
            row = lambda ref: ref[p[0] : p[0] + 1, pl.ds(p[1], width)]
            w = jnp.exp2(s * (SCALE * LOG2E) - row(lse_ref) * LOG2E)
            if p in masked:
                w = jnp.where(lax.broadcasted_iota(jnp.int32, s.shape, 1) >= lax.broadcasted_iota(jnp.int32, s.shape, 0), w, 0.0)
            ds = (w * (dp - row(delta_ref))).astype(LOW)
            dv_s[here, :] += _dot(w.astype(LOW), do)
            dk_s[here, :] += _dot(ds, q)
            dq_s[:, pl.ds(p[0] * bq + p[1], width)] += _dot(kt, ds)

    _blocks(block, pieces, i, bq // width)
    for n in range(heads):
        dq_ref[n] = (dq_s[:, pl.ds(n * bq, bq)] * SCALE).T.astype(LOW)

    @pl.when(i == pl.num_programs(0) - 1)
    def _():
        dk_ref[...] = (dk_s[...] * SCALE).astype(LOW)
        dv_ref[...] = dv_s[...].astype(LOW)


def attend_back(q, k, v, do, lse, delta, bq=1024, width=256):
    heads, t, d = q.shape
    block, whole = pl.BlockSpec((heads, bq, d), lambda i: (0, i, 0)), pl.BlockSpec((t, d), lambda i: (0, 0))
    row = pl.BlockSpec((heads, bq), lambda i: (0, i))
    return pl.pallas_call(
        functools.partial(_attend_back, width=width),
        grid=(t // bq,),
        in_specs=[block, whole, whole, block, row, row],
        out_specs=[block, whole, whole],
        out_shape=[jax.ShapeDtypeStruct(a.shape, LOW) for a in (q, k, v)],
        scratch_shapes=[pltpu.VMEM((d, heads * bq), WIDE), pltpu.VMEM((t, d), WIDE), pltpu.VMEM((t, d), WIDE)],
        compiler_params=pltpu.CompilerParams(dimension_semantics=("arbitrary",), vmem_limit_bytes=VMEM),
        cost_estimate=pl.CostEstimate(flops=10 * heads * t * t * d, transcendentals=heads * t * t, bytes_accessed=9 * heads * t * d),
        name="attend_back",
    )(q, k, v, do, lse, delta)


AXES = (8, 4, 2)
ORDERS = ((0, 1, 2), (1, 2, 0), (2, 0, 1))


def normed(h):
    wide = h.astype(jnp.float32)
    scale = lax.rsqrt(jnp.mean(wide**2, -1, keepdims=True) + 1e-6)
    return (wide * scale).astype(jnp.bfloat16)


def by_normed(h, by_b):
    h, by_b = h.astype(WIDE), by_b.astype(LOW).astype(WIDE)
    scale = lax.rsqrt(jnp.mean(h * h, -1, keepdims=True) + 1e-6)
    return by_b * scale - h * (scale * scale * scale * jnp.mean(by_b * h, -1, keepdims=True))


def angles(tokens):
    half = HEAD // 2
    angle = np.arange(tokens, dtype=np.float32)[:, None] * np.float32(THETA) ** (-np.arange(half, dtype=np.float32) / np.float32(half))
    return jnp.asarray(np.concatenate([np.cos(angle), np.sin(angle)], -1).astype(np.float32))


def _cos_sin(table):
    half = HEAD // 2
    other = pltpu.roll(table, half, 1)
    first = lax.broadcasted_iota(jnp.int32, table.shape, 1) < half
    return jnp.where(first, table, other), jnp.where(first, -other, table)


def _turn(t, cos, sin):
    wide = t.astype(WIDE)
    return (wide * cos + pltpu.roll(wide, HEAD // 2, 1) * sin).astype(LOW)


def _before(h_ref, turn_ref, wq_ref, wk_ref, wv_ref, q_ref, k_ref, v_ref):
    a = normed(h_ref[...])
    cos, sin = _cos_sin(turn_ref[...])
    q = _dot(a, wq_ref[...]).astype(LOW)
    for n in range(q_ref.shape[0]):
        q_ref[n] = _turn(q[:, n * HEAD : (n + 1) * HEAD], cos, sin)
    kv = _dot(a, jnp.concatenate([wk_ref[...], wv_ref[...]], 1)).astype(LOW)
    k_ref[...] = _turn(kv[:, :HEAD], cos, sin)
    v_ref[...] = kv[:, HEAD:]


def _of_layer(number, w):
    return pl.BlockSpec((None, *w.shape[1:]), lambda *_: (number, 0, 0))


def before(number, h, turns, wq, wk, wv, tb=512):
    t, d = h.shape
    heads = wq.shape[2] // HEAD
    row = lambda i: (i, 0)
    return pl.pallas_call(
        _before,
        grid=(t // tb,),
        in_specs=[pl.BlockSpec((tb, d), row), pl.BlockSpec((tb, HEAD), row), *(_of_layer(number, w) for w in (wq, wk, wv))],
        out_specs=[pl.BlockSpec((heads, tb, HEAD), lambda i: (0, i, 0)), pl.BlockSpec((tb, HEAD), row), pl.BlockSpec((tb, HEAD), row)],
        out_shape=[jax.ShapeDtypeStruct((heads, t, HEAD), LOW), jax.ShapeDtypeStruct((t, HEAD), LOW), jax.ShapeDtypeStruct((t, HEAD), LOW)],
        compiler_params=pltpu.CompilerParams(dimension_semantics=("arbitrary",), vmem_limit_bytes=VMEM),
        cost_estimate=pl.CostEstimate(flops=2 * t * d * (heads + 2) * HEAD, transcendentals=t, bytes_accessed=4 * t * d),
        name="before",
    )(h, turns, wq, wk, wv)


def _halve(core, acc_s, refs):
    if len(refs) == 1:
        refs[0][...] = acc_s[...].astype(LOW)
        return
    rows = refs[0].shape[1]
    for n in range(8):
        for to, at in zip(refs, (core, 1 - core)):
            to[n] = acc_s[pl.ds(pl.multiple_of((2 * n + at) * rows, 8), rows), :].astype(LOW)


def _gradient(rows, columns, halves):
    return [jax.ShapeDtypeStruct((8, rows // 16, columns), LOW)] * 2 if halves else [jax.ShapeDtypeStruct((rows, columns), LOW)]


def _at_start(shapes):
    return [pl.BlockSpec(one.shape, lambda i, n=len(one.shape): (0,) * n) for one in shapes]


def _after_back(core_ref, dmid_ref, att_ref, wo_ref, datt_ref, delta_ref, *rest):
    *out_refs, acc_s = rest
    i = pl.program_id(0)
    dmid = dmid_ref[...]
    heads = att_ref.shape[0]
    datt = _dot(dmid, wo_ref[...], cb=1).astype(LOW)
    for n in range(heads):
        one = datt[:, n * HEAD : (n + 1) * HEAD]
        datt_ref[n] = one
        delta_ref[n : n + 1, :] = (one.astype(WIDE) * att_ref[n].astype(WIDE)).T.sum(0, keepdims=True)
    term = jnp.concatenate([_dot(att_ref[n].T, dmid) for n in range(heads)], 0)

    @pl.when(i == 0)
    def _():
        acc_s[...] = term

    @pl.when(i > 0)
    def _():
        acc_s[...] += term

    @pl.when(i == pl.num_programs(0) - 1)
    def _():
        _halve(core_ref[0], acc_s, out_refs)


def after_back(number, core, dmid, att, wo, halves, tb=512):
    t, d = dmid.shape
    heads = att.shape[0]
    head = pl.BlockSpec((heads, tb, HEAD), lambda i: (0, i, 0))
    grad = _gradient(heads * HEAD, d, halves)
    return pl.pallas_call(
        _after_back,
        grid=(t // tb,),
        in_specs=[pl.BlockSpec(memory_space=pltpu.SMEM), pl.BlockSpec((tb, d), lambda i: (i, 0)), head, _of_layer(number, wo)],
        out_specs=[head, pl.BlockSpec((heads, tb), lambda i: (0, i)), *_at_start(grad)],
        out_shape=[jax.ShapeDtypeStruct(att.shape, LOW), jax.ShapeDtypeStruct((heads, t), WIDE), *grad],
        scratch_shapes=[pltpu.VMEM((heads * HEAD, d), WIDE)],
        compiler_params=pltpu.CompilerParams(dimension_semantics=("arbitrary",), vmem_limit_bytes=VMEM),
        cost_estimate=pl.CostEstimate(flops=4 * t * d * heads * HEAD, transcendentals=0, bytes_accessed=8 * t * d),
        name="after_back",
    )(core, dmid, att, wo)


def _before_back(core_ref, h_ref, turn_ref, dq_ref, dk_ref, dv_ref, *rest, inner):
    if inner:
        dmid_ref, wq_ref, wk_ref, wv_ref, dh_ref, *rest = rest
    *out_refs, acc_s = rest
    i = pl.program_id(0)
    cos, sin = _cos_sin(turn_ref[...])
    sin = -sin
    by = jnp.concatenate([_turn(dq_ref[n], cos, sin) for n in range(dq_ref.shape[0])] + [_turn(dk_ref[...], cos, sin), dv_ref[...]], 1)
    term = _dot(normed(h_ref[...]).T, by)

    @pl.when(i == 0)
    def _():
        acc_s[...] = term

    @pl.when(i > 0)
    def _():
        acc_s[...] += term

    if inner:
        w = jnp.concatenate([wq_ref[...], wk_ref[...], wv_ref[...]], 1)
        dh_ref[...] = (dmid_ref[...].astype(WIDE) + by_normed(h_ref[...], _dot(by, w, cb=1))).astype(LOW)

    @pl.when(i == pl.num_programs(0) - 1)
    def _():
        _halve(core_ref[0], acc_s, out_refs)


def before_back(number, core, h, turns, dq, dk, dv, dmid, wq, wk, wv, inner, halves, tb=512):
    t, d = h.shape
    heads = dq.shape[0]
    wide = (heads + 2) * HEAD
    row = lambda i: (i, 0)
    states, head = pl.BlockSpec((tb, d), row), pl.BlockSpec((tb, HEAD), row)
    grad = _gradient(d, wide, halves)
    more = [states, *(_of_layer(number, w) for w in (wq, wk, wv))] if inner else []
    return pl.pallas_call(
        functools.partial(_before_back, inner=inner),
        grid=(t // tb,),
        in_specs=[pl.BlockSpec(memory_space=pltpu.SMEM), states, head, pl.BlockSpec((heads, tb, HEAD), lambda i: (0, i, 0)), head, head, *more],
        out_specs=([states] if inner else []) + _at_start(grad),
        out_shape=([jax.ShapeDtypeStruct((t, d), LOW)] if inner else []) + grad,
        scratch_shapes=[pltpu.VMEM((d, wide), WIDE)],
        compiler_params=pltpu.CompilerParams(dimension_semantics=("arbitrary",), vmem_limit_bytes=VMEM),
        cost_estimate=pl.CostEstimate(flops=(4 if inner else 2) * t * d * wide, transcendentals=t, bytes_accessed=10 * t * d),
        name="before_back",
    )(core, h, turns, dq, dk, dv, *([dmid, wq, wk, wv] if inner else []))


def _mlp_forward(h_ref, att_ref, wo_ref, wg_ref, wu_ref, wd_ref, mid_ref, y_ref, gate_ref, up_ref, b_s, mid_s, acc_s, *, tb, strip):
    j, i = pl.program_id(0), pl.program_id(1)
    last = pl.num_programs(0) - 1
    for at in range(0, tb, strip):
        here = pl.ds(pl.multiple_of(i * tb + at, strip), strip)
        cut = pl.ds(at, strip)

        @pl.when(j == 0)
        def _():
            mid = (h_ref[cut, :].astype(WIDE) + _dot(jnp.concatenate([att_ref[n, cut, :] for n in range(att_ref.shape[0])], 1), wo_ref[...]).astype(LOW).astype(WIDE)).astype(LOW)
            mid_ref[cut, :] = mid
            mid_s[here, :] = mid
            b_s[here, :] = normed(mid)
            acc_s[here, :] = jnp.zeros((strip, acc_s.shape[1]), WIDE)

    here = [pl.ds(pl.multiple_of(i * tb + at, strip), strip) for at in range(0, tb, strip)]
    both = lambda n: [_dot(b_s[here[n], :], w[...]) for w in (wg_ref, wu_ref)]
    ahead = both(0)
    for n in range(len(here)):
        gate, up = ahead
        ahead = both(n + 1) if n + 1 < len(here) else None
        cut = pl.ds(n * strip, strip)
        gate_ref[cut, :] = gate
        up_ref[cut, :] = up
        t = (gate * (0.5 * jnp.tanh(0.5 * gate) + 0.5) * up).astype(LOW)
        acc_s[here[n], :] += _dot(t, wd_ref[...])

    @pl.when(j == last)
    def _():
        here = pl.ds(pl.multiple_of(i * tb, tb), tb)
        y_ref[...] = (mid_s[here, :].astype(WIDE) + acc_s[here, :].astype(LOW).astype(WIDE)).astype(LOW)


def _of_mlp(number, d, fb):
    side = pl.BlockSpec((None, d, fb), lambda j, i: (number, 0, j))
    return side, side, pl.BlockSpec((None, fb, d), lambda j, i: (number, j, 0))


def mlp_forward(number, h, att, wo, wg, wu, wd, tb=1024, fb=512, strip=256):
    t, d = h.shape
    ff, hd = wg.shape[2], wo.shape[1]
    n = t // tb
    at_first = lambda j, i: (jnp.where(j == 0, i, n - 1), 0)
    at_last = lambda j, i: (jnp.where(j == ff // fb - 1, i, 0), 0)
    return pl.pallas_call(
        functools.partial(_mlp_forward, tb=tb, strip=strip),
        grid=(ff // fb, n),
        in_specs=[pl.BlockSpec((tb, d), at_first), pl.BlockSpec((att.shape[0], tb, HEAD), lambda j, i: (0, at_first(j, i)[0], 0)), _of_layer(number, wo),
                  *_of_mlp(number, d, fb)],
        out_specs=[pl.BlockSpec((tb, d), at_first), pl.BlockSpec((tb, d), at_last),
                   *[pl.BlockSpec((tb, fb), lambda j, i: (i, j))] * 2],
        scratch_shapes=[pltpu.VMEM((t, d), LOW), pltpu.VMEM((t, d), LOW), pltpu.VMEM((t, d), WIDE)],
        out_shape=[jax.ShapeDtypeStruct((t, d), LOW), jax.ShapeDtypeStruct((t, d), LOW), jax.ShapeDtypeStruct((t, ff), WIDE),
                   jax.ShapeDtypeStruct((t, ff), WIDE)],
        compiler_params=pltpu.CompilerParams(dimension_semantics=("arbitrary", "arbitrary"), vmem_limit_bytes=VMEM),
        cost_estimate=pl.CostEstimate(flops=2 * t * d * (3 * ff + hd), transcendentals=t * ff, bytes_accessed=8 * t * ff + 6 * d * ff + 10 * t * d),
        name="mlp_forward",
    )(h, att, wo, wg, wu, wd)


def _mlp_backward(core_ref, dy_ref, mid_ref, gate_ref, up_ref, wg_ref, wu_ref, wd_ref, dmid_ref, *rest, tb, strip):
    *out_refs, bt_s, dyt_s, db_s, pg_s, pu_s, t_s, ag_s, au_s, ad_s = rest
    per = len(out_refs) // 3
    j, i = pl.program_id(0), pl.program_id(1)
    all_i = pl.ds(pl.multiple_of(i * tb, tb), tb)

    @pl.when(j == 0)
    def _():
        for at in range(0, tb, strip):
            here = pl.ds(pl.multiple_of(i * tb + at, strip), strip)
            bt_s[:, here] = normed(mid_ref[here, :]).T
            dyt_s[:, here] = dy_ref[here, :].T
            db_s[here, :] = jnp.zeros((strip, db_s.shape[1]), WIDE)

    @pl.when(i == 0)
    def _():
        for ref in (ag_s, au_s, ad_s):
            ref[...] = jnp.zeros_like(ref)

    for at in range(0, tb, strip):
        here = pl.ds(pl.multiple_of(i * tb + at, strip), strip)
        cut = pl.ds(at, strip)
        dt = _dot(dy_ref[here, :], wd_ref[...], cb=1).astype(LOW).astype(WIDE)
        gate, up = gate_ref[cut, :], up_ref[cut, :]
        half = 0.5 * jnp.tanh(0.5 * gate)
        sig = half + 0.5
        silu = gate * sig
        by_up = (dt * silu).astype(LOW)
        by_gate = (dt * up * (sig + silu * (0.5 - half))).astype(LOW)
        t_s[cut, :] = (silu * up).astype(LOW)
        pg_s[cut, :] = by_gate
        pu_s[cut, :] = by_up
        db_s[here, :] += _dot(by_gate, wg_ref[...], cb=1) + _dot(by_up, wu_ref[...], cb=1)

    ag_s[...] += _dot(bt_s[:, all_i], pg_s[...])
    au_s[...] += _dot(bt_s[:, all_i], pu_s[...])
    ad_s[...] += _dot(dyt_s[:, all_i], t_s[...])

    @pl.when(i == pl.num_programs(1) - 1)
    def _():
        core = core_ref[0]
        _halve(core, ag_s, out_refs[:per])
        _halve(core, au_s, out_refs[per : 2 * per])
        down = out_refs[2 * per :]
        if per == 1:
            down[0][...] = ad_s[...].T.astype(LOW)
        else:
            wide = down[0].shape[1]
            for to, at in zip(down, (core, 1 - core)):
                to[0] = ad_s[:, pl.ds(pl.multiple_of(at * wide, 128), wide)].T.astype(LOW)

    @pl.when(j == pl.num_programs(0) - 1)
    def _():
        for at in range(0, tb, strip):
            here = pl.ds(pl.multiple_of(i * tb + at, strip), strip)
            cut = pl.ds(at, strip)
            dmid_ref[cut, :] = (dy_ref[here, :].astype(WIDE) + by_normed(mid_ref[here, :], db_s[here, :])).astype(LOW)


def mlp_backward(number, core, dy, mid, gate, up, wg, wu, wd, halves, tb=1024, strip=256):
    t, d = dy.shape
    ff = wg.shape[2]
    n, fb = t // tb, ff // 8
    whole = lambda j, i: (0, 0)
    at_last = lambda j, i: (jnp.where(j == 7, i, 0), 0)
    rows = d // 16
    if halves:
        side, tall = [pl.BlockSpec((8, rows, fb), lambda j, i: (0, 0, j))] * 2, [pl.BlockSpec((1, fb // 2, d), lambda j, i: (j, 0, 0))] * 2
    else:
        side, tall = [pl.BlockSpec((d, fb), lambda j, i: (0, j))], [pl.BlockSpec((fb, d), lambda j, i: (j, 0))]
    one = pl.Buffered(1)
    return pl.pallas_call(
        functools.partial(_mlp_backward, tb=tb, strip=strip),
        grid=(8, n),
        in_specs=[pl.BlockSpec(memory_space=pltpu.SMEM), pl.BlockSpec((t, d), whole, pipeline_mode=one), pl.BlockSpec((t, d), whole, pipeline_mode=one),
                  *[pl.BlockSpec((tb, fb), lambda j, i: (i, j))] * 2,
                  *_of_mlp(number, d, fb)],
        out_specs=[pl.BlockSpec((tb, d), at_last), *side, *side, *tall],
        scratch_shapes=[pltpu.VMEM((d, t), LOW), pltpu.VMEM((d, t), LOW), pltpu.VMEM((t, d), WIDE)] + [pltpu.VMEM((tb, fb), LOW)] * 3
        + [pltpu.VMEM((d, fb), WIDE)] * 3,
        out_shape=[jax.ShapeDtypeStruct((t, d), LOW), *_gradient(d, ff, halves), *_gradient(d, ff, halves), *_gradient(ff, d, halves)],
        compiler_params=pltpu.CompilerParams(dimension_semantics=("arbitrary", "arbitrary"), vmem_limit_bytes=VMEM),
        cost_estimate=pl.CostEstimate(flops=12 * t * d * ff, transcendentals=t * ff, bytes_accessed=8 * t * ff + 12 * d * ff + 6 * t * d),
        name="mlp_backward",
    )(core, dy, mid, gate, up, wg, wu, wd)


def swapped(t, step):
    return lax.ppermute(t, "dp", [(n, n ^ step) for n in range(16)])


class Reduction:
    def __init__(self, place, pairs, orders):
        self.place, self.orders, self.at = place, orders, 0
        self.held = [[keep.reshape(2, 2, 2, *keep.shape[1:])] for keep, _ in pairs]
        self.out = [send for _, send in pairs]

    def go(self):
        self.got = [swapped(t, AXES[order[self.at - 1]] if self.at else 1) for t, order in zip(self.out, self.orders)]

    def take(self):
        total = lambda parts: functools.reduce(jnp.add, [p.astype(WIDE) for p in parts]).astype(LOW)
        for n, order in enumerate(self.orders[: len(self.out)]):
            self.held[n].append(self.got[n].reshape(self.held[n][0].shape))
            if self.at == 3:
                self.out[n] = total(self.held[n]).reshape(self.held[n][0].shape[3:])
                continue
            axis = order[self.at]
            mine = self.place // AXES[axis] % 2
            pick = lambda t, at: lax.dynamic_index_in_dim(t, at, axis, keepdims=True)
            self.out[n] = total([pick(t, 1 - mine) for t in self.held[n]])
            self.held[n] = [pick(t, mine) for t in self.held[n]]
        self.at += 1


def landed(x, *reductions):
    x, got = lax.optimization_barrier((x, [r.got for r in reductions]))
    for r, new in zip(reductions, got):
        r.got = new
        r.take()
    x, out = lax.optimization_barrier((x, [r.out for r in reductions]))
    for r, new in zip(reductions, out):
        r.out = new
        if r.at < 4:
            r.go()
    return x


MESH_ID = pl.DeviceIdType.MESH


def _squares(*refs):
    *in_refs, o_ref, own_s, all_s, send_sem, recv_sem = refs
    me = lax.axis_index("dp")
    barrier = pltpu.get_barrier_semaphore()
    for n in range(1, 16):
        pl.semaphore_signal(barrier, inc=1, device_id={"dp": (me + n) % 16}, device_id_type=MESH_ID)
    total = jnp.zeros(own_s.shape, WIDE)
    for ref in in_refs:
        x = ref[...].astype(WIDE)
        x = (x * x).reshape(-1, 8, x.shape[1]).sum(0)
        for at in range(0, x.shape[1], 128):
            total += x[:, at : at + 128]
    own_s[...] = total
    pl.semaphore_wait(barrier, 15)
    copies = [pltpu.make_async_remote_copy(src_ref=own_s, dst_ref=all_s.at[n], send_sem=send_sem.at[n], recv_sem=recv_sem.at[n],
                                           device_id={"dp": (me + n) % 16}, device_id_type=MESH_ID) for n in range(1, 16)]
    for copy in copies:
        copy.start()
    for copy in copies:
        copy.wait()
    for n in range(1, 16):
        total += all_s[n]
    o_ref[...] = jnp.broadcast_to(jnp.sum(total, keepdims=True), o_ref.shape)


def squares(arrays):
    vmem = pl.BlockSpec(memory_space=pltpu.VMEM)
    tile = (8, 128)
    return pl.pallas_call(
        _squares,
        in_specs=[vmem] * len(arrays),
        out_specs=vmem,
        out_shape=jax.ShapeDtypeStruct(tile, WIDE),
        scratch_shapes=[pltpu.VMEM(tile, WIDE), pltpu.VMEM((16, *tile), WIDE), pltpu.SemaphoreType.DMA((16,)), pltpu.SemaphoreType.DMA((16,))],
        compiler_params=pltpu.CompilerParams(collective_id=0, has_side_effects=True),
        name="squares",
    )(*arrays)


def _gathered(*refs, turns):
    n = len(turns)
    ins, outs = refs[:n], refs[n : 2 * n]
    ici_send, ici_recv, pair_send, pair_recv, own_sem = refs[2 * n :]
    me = lax.axis_index("dp")
    steps = [s * (1 - 2 * (me // s % 2)) for s in AXES]
    other = 1 - 2 * (me % 2)
    barrier = pltpu.get_barrier_semaphore()
    for step in (*steps, other):
        pl.semaphore_signal(barrier, inc=1, device_id={"dp": me + step}, device_id_type=MESH_ID)
    pl.semaphore_wait(barrier, 4)

    def block(mask):
        return me + sum(steps[a] for a in range(3) if mask >> a & 1)

    def copy(k, mask, to, sems, row):
        src = ins[k] if mask == 0 else outs[k].at[:, block(mask)]
        return pltpu.make_async_remote_copy(src_ref=src, dst_ref=outs[k].at[:, block(mask)], send_sem=sems[0].at[k, row], recv_sem=sems[1].at[k, row],
                                            device_id={"dp": me + to}, device_id_type=MESH_ID)

    started = []

    def go(k, mask):
        order = ORDERS[turns[k]]
        last = max([order.index(a) for a in range(3) if mask >> a & 1], default=-1)
        for a in order[last + 1 :]:
            one = copy(k, mask, steps[a], (ici_send, ici_recv), mask | 1 << a)
            one.start()
            started.append(one)
        one = copy(k, mask, other, (pair_send, pair_recv), mask)
        one.start()
        started.append(one)

    def here(k, mask):
        copy(k, mask, steps[0], (ici_send, ici_recv), mask).wait_recv()
        go(k, mask)

    mine = [pltpu.make_async_copy(ins[k], outs[k].at[:, me], own_sem.at[k]) for k in range(n)]
    for k in range(n):
        go(k, 0)
    for one in mine:
        one.start()
    bit = lambda k, *at: sum(1 << ORDERS[turns[k]][a] for a in at)
    for sets in (((0,), (1,), (2,)), ((0, 1), (0, 2), (1, 2)), ((0, 1, 2),)):
        for k in range(n):
            for at in sets:
                here(k, bit(k, *at))
    for k in range(n):
        for mask in range(8):
            copy(k, mask, other, (pair_send, pair_recv), mask).wait_recv()
    for one in started:
        one.wait_send()
    for one in mine:
        one.wait()


def gathered(blocks, turns):
    hbm = pl.BlockSpec(memory_space=pl.ANY)
    n = len(blocks)
    sems = [pltpu.SemaphoreType.DMA((n, 8))] * 4 + [pltpu.SemaphoreType.DMA((n,))]
    return pl.pallas_call(
        functools.partial(_gathered, turns=turns),
        in_specs=[hbm] * n,
        out_specs=[hbm] * n,
        out_shape=[jax.ShapeDtypeStruct((b.shape[0], 16, *b.shape[1:]), b.dtype) for b in blocks],
        scratch_shapes=sems,
        compiler_params=pltpu.CompilerParams(collective_id=1, has_side_effects=True, vmem_limit_bytes=2**20),
        name="gathered",
    )(*blocks)


def _settled(*refs):
    n = len(refs) // 2
    copies = [pltpu.make_async_copy(refs[k], refs[n + k], refs[-1].at[k]) for k in range(n)]
    for copy in copies:
        copy.start()
    for copy in copies:
        copy.wait()


def settled(arrays):
    hbm = pl.BlockSpec(memory_space=pl.ANY)
    n = len(arrays)
    return pl.pallas_call(
        _settled,
        in_specs=[hbm] * n,
        out_specs=[hbm] * n,
        out_shape=[jax.ShapeDtypeStruct(a.shape, a.dtype) for a in arrays],
        scratch_shapes=[pltpu.SemaphoreType.DMA((n,))],
        compiler_params=pltpu.CompilerParams(vmem_limit_bytes=2**20),
        name="settled",
    )(*arrays)


def adamw(w, m, v, g):
    m = 0.9 * m + 0.1 * g
    v = 0.95 * v + 0.05 * g * g
    step = m * lax.rsqrt(v + 1e-8) + 0.1 * w
    return (w - 0.02 * step).astype(jnp.bfloat16), m, v


def clipped(gradients, sum_of_squares, count):
    factor = jnp.minimum(1.0, 0.5 * lax.rsqrt(sum_of_squares / count + 1e-30))
    return [g * factor for g in gradients]


def solution(mesh):
    def step(x, dy, *arrays):
        weights, m, v = (arrays[i : i + 7] for i in (0, 7, 14))
        layers = weights[0].shape[0]
        me = lax.axis_index("dp")
        core = (me % 2).astype(jnp.int32).reshape(1)
        wq, wk, wv, wo, wg, wu, wd = weights
        turns = angles(x.shape[1])
        h, kept = x[0], []
        for number in range(layers):
            q, k, val = before(number, h, turns, wq, wk, wv)
            att, lse = attend(q, k, val)
            mid, y, gate, up = mlp_forward(number, h, att, wo, wg, wu, wd)
            kept.append((h, q, k, val, att, lse, mid, gate, up))
            h = y
        by_h = dy[0]
        scattered = lambda t: lax.psum_scatter(t, "dp", scatter_dimension=0, tiled=True)
        dq, dk = wq.shape[2], wk.shape[2]
        late_mlp, late_small = [], []
        for number in reversed(range(layers)):
            h, q, k, val, att, lse, mid, gate, up = kept[number]
            last = number == 0
            by_mid, *by_mlp = mlp_backward(number, core, by_h, mid, gate, up, wg, wu, wd, last)
            if last:
                big = Reduction(me, [by_mlp[n : n + 2] for n in (0, 2, 4)], ORDERS)
                big.go()
                by_mid, late_small, sides = lax.optimization_barrier((by_mid, late_small, [m[:2] for m in late_mlp]))
                late_small = [scattered(some) for some in late_small]
            by_att, delta, *by_o = after_back(number, core, by_mid, att, wo, last)
            if last:
                by_att = landed(by_att, big)
                out = Reduction(me, [by_o], ORDERS[1:])
                out.go()
            by_q, by_k, by_v = attend_back(q, k, val, by_att, lse, delta)
            if last:
                by_q, downs = lax.optimization_barrier((landed(by_q, big, out), [m[2] for m in late_mlp]))
            outs = before_back(number, core, h, turns, by_q, by_k, by_v, by_mid, wq, wk, wv, not last, last)
            if not last:
                by_h, by_qkv = outs
                late_mlp.append([scattered(t) for t in by_mlp])
                by_o = by_o[0].reshape(16, -1, by_o[0].shape[1])
                by_qkv = by_qkv.reshape(16, -1, by_qkv.shape[1])
                wider = ((0, 0), (0, 0), (0, by_qkv.shape[2] - by_o.shape[2]))
                late_small.append(jnp.concatenate([by_qkv, jnp.pad(by_o, wider)], 1).reshape(-1, by_qkv.shape[2]))
        small = Reduction(me, [outs], ORDERS)
        small.go()
        for r in (big, small, out):
            while r.at < 4:
                r.take()
                if r.at < 4:
                    r.go()
        rows = wq.shape[1] // 16
        mine = [[*small.out, *out.out, *big.out]]
        mine += [[some[:rows], some[rows:, : wo.shape[2]], *side, down] for some, side, down in zip(late_small, sides, downs)][::-1]
        total = squares([t for some in mine for t in some])[0, 0]
        mine = [[qkv[:, :dq], qkv[:, dq : dq + dk], qkv[:, dq + dk :], *rest] for qkv, *rest in mine]
        gradients = [jnp.stack([some[i] for some in mine]).astype(WIDE) for i in range(7)]
        gradients = clipped(gradients, total, 16 * sum(g.size for g in gradients))
        own = [lax.dynamic_slice_in_dim(w, me * one.shape[1], one.shape[1], 1).astype(jnp.float32) for w, one in zip(weights, m, strict=True)]
        new = [adamw(w, m, v, g) for w, m, v, g in zip(own, m, v, gradients, strict=True)]
        whole = gathered([one[0] for one in new], (0, 1, 1, 2, 0, 1, 2))
        whole = [t.reshape(t.shape[0], -1, t.shape[3]) for t in settled(whole)]
        return (*whole, *(one[1] for one in new), *(one[2] for one in new))

    states, all_of, cut = P(("rep", "dp"), None, None), P(None, None, None), P(None, "dp", None)
    return jax.shard_map(
        step,
        mesh=mesh,
        in_specs=(states, states) + (all_of,) * 7 + (cut,) * 14,
        out_specs=(P("rep", None, None),) * 7 + (P("rep", "dp", None),) * 14,
        check_vma=False,
    )
```

```python
import functools

import jax
import jax.numpy as jnp
import numpy as np
from jax import lax
from jax.experimental import pallas as pl
from jax.experimental.pallas import tpu as pltpu
from jax.sharding import PartitionSpec as P

LOW = jnp.bfloat16
WIDE = jnp.float32
LOG2E = 1.4426950408889634
VMEM = 56 * 2**20
NEG = -1e30
HEAD = 128
SCALE = HEAD**-0.5
THETA = 10000


def _dot(a, b, ca=1, cb=0):
    return lax.dot_general(a, b, (((ca,), (cb,)), ((), ())), preferred_element_type=WIDE)


def _strips(q_ref, width):
    return [(n, at, at // width) for n in range(q_ref.shape[0]) for at in range(0, q_ref.shape[1], width)]


def _blocks(block, pieces, i, per):
    lax.fori_loop(0, i * per, lambda j, _: block(j, pieces, ()), None)
    for n in range(per):
        block(i * per + n, [p for p in pieces if p[2] >= n], [p for p in pieces if p[2] == n])


def _attend(q_ref, k_ref, v_ref, o_ref, lse_ref, top_s, mix_s, *, width):
    heads, bq, d = q_ref.shape
    pieces = _strips(q_ref, width)
    e = SCALE * LOG2E
    column = lambda p: pl.ds(p[0] * bq + p[1], width)
    top_s[...] = jnp.full(top_s.shape, NEG, WIDE)
    mix_s[...] = jnp.zeros(mix_s.shape, WIDE)
    ones = jnp.ones((8, width), LOW)

    def block(j, some, masked):
        here = pl.ds(pl.multiple_of(j * width, width), width)
        k = k_ref[here, :]
        values = jnp.concatenate([v_ref[here, :].T, ones], axis=0)
        scores = [_dot(k, q_ref[p[0], pl.ds(p[1], width), :], cb=1) for p in some]
        weights, keeps = [], []
        for p, s in zip(some, scores):
            if p in masked:
                s = jnp.where(lax.broadcasted_iota(jnp.int32, s.shape, 1) >= lax.broadcasted_iota(jnp.int32, s.shape, 0), s, 2 * NEG)
            old = top_s[:, column(p)]
            top = jnp.maximum(old, s.max(axis=0, keepdims=True))
            top_s[:, column(p)] = top
            weights.append(jnp.exp2((s - top) * e).astype(LOW))
            keeps.append(jnp.exp2((old - top) * e))
        for p, w, keep in zip(some, weights, keeps):
            mix_s[:, column(p)] = mix_s[:, column(p)] * keep + _dot(values, w)

    _blocks(block, pieces, pl.program_id(0), bq // width)
    for n in range(heads):
        cut = pl.ds(n * bq, bq)
        total = mix_s[d : d + 1, cut]
        o_ref[n] = (mix_s[:d, cut] * (1 / total)).T.astype(LOW)
        lse_ref[n : n + 1, :] = top_s[:, cut] * SCALE + jnp.log(total)


def attend(q, k, v, bq=1024, width=512):
    heads, t, d = q.shape
    block, whole = pl.BlockSpec((heads, bq, d), lambda i: (0, i, 0)), pl.BlockSpec((t, d), lambda i: (0, 0))
    return pl.pallas_call(
        functools.partial(_attend, width=width),
        grid=(t // bq,),
        in_specs=[block, whole, whole],
        out_specs=[block, pl.BlockSpec((heads, bq), lambda i: (0, i))],
        out_shape=[jax.ShapeDtypeStruct(q.shape, LOW), jax.ShapeDtypeStruct((heads, t), WIDE)],
        scratch_shapes=[pltpu.VMEM((1, heads * bq), WIDE), pltpu.VMEM((d + 8, heads * bq), WIDE)],
        compiler_params=pltpu.CompilerParams(dimension_semantics=("arbitrary",), vmem_limit_bytes=VMEM),
        cost_estimate=pl.CostEstimate(flops=4 * heads * t * t * d, transcendentals=heads * t * t, bytes_accessed=6 * heads * t * d),
        name="attend",
    )(q, k, v)


def _attend_back(q_ref, k_ref, v_ref, do_ref, lse_ref, delta_ref, dq_ref, dk_ref, dv_ref, dq_s, dk_s, dv_s, *, width):
    heads, bq, d = q_ref.shape
    pieces = _strips(q_ref, width)
    i = pl.program_id(0)

    @pl.when(i == 0)
    def _():
        dk_s[...] = jnp.zeros_like(dk_s)
        dv_s[...] = jnp.zeros_like(dv_s)

    dq_s[...] = jnp.zeros_like(dq_s)

    def block(j, some, masked):
        here = pl.ds(pl.multiple_of(j * width, width), width)
        k, v = k_ref[here, :], v_ref[here, :]
        kt = k.T
        qs = [q_ref[p[0], pl.ds(p[1], width), :] for p in some]
        dos = [do_ref[p[0], pl.ds(p[1], width), :] for p in some]
        scores = [_dot(k, x, cb=1) for x in qs]
        dps = [_dot(v, x, cb=1) for x in dos]
        for p, q, do, s, dp in zip(some, qs, dos, scores, dps):
            row = lambda ref: ref[p[0] : p[0] + 1, pl.ds(p[1], width)]
            w = jnp.exp2(s * (SCALE * LOG2E) - row(lse_ref) * LOG2E)
            if p in masked:
                w = jnp.where(lax.broadcasted_iota(jnp.int32, s.shape, 1) >= lax.broadcasted_iota(jnp.int32, s.shape, 0), w, 0.0)
            ds = (w * (dp - row(delta_ref))).astype(LOW)
            dv_s[here, :] += _dot(w.astype(LOW), do)
            dk_s[here, :] += _dot(ds, q)
            dq_s[:, pl.ds(p[0] * bq + p[1], width)] += _dot(kt, ds)

    _blocks(block, pieces, i, bq // width)
    for n in range(heads):
        dq_ref[n] = (dq_s[:, pl.ds(n * bq, bq)] * SCALE).T.astype(LOW)

    @pl.when(i == pl.num_programs(0) - 1)
    def _():
        dk_ref[...] = (dk_s[...] * SCALE).astype(LOW)
        dv_ref[...] = dv_s[...].astype(LOW)


def attend_back(q, k, v, do, lse, delta, bq=1024, width=256):
    heads, t, d = q.shape
    block, whole = pl.BlockSpec((heads, bq, d), lambda i: (0, i, 0)), pl.BlockSpec((t, d), lambda i: (0, 0))
    row = pl.BlockSpec((heads, bq), lambda i: (0, i))
    return pl.pallas_call(
        functools.partial(_attend_back, width=width),
        grid=(t // bq,),
        in_specs=[block, whole, whole, block, row, row],
        out_specs=[block, whole, whole],
        out_shape=[jax.ShapeDtypeStruct(a.shape, LOW) for a in (q, k, v)],
        scratch_shapes=[pltpu.VMEM((d, heads * bq), WIDE), pltpu.VMEM((t, d), WIDE), pltpu.VMEM((t, d), WIDE)],
        compiler_params=pltpu.CompilerParams(dimension_semantics=("arbitrary",), vmem_limit_bytes=VMEM),
        cost_estimate=pl.CostEstimate(flops=10 * heads * t * t * d, transcendentals=heads * t * t, bytes_accessed=9 * heads * t * d),
        name="attend_back",
    )(q, k, v, do, lse, delta)


AXES = (8, 4, 2)
ORDERS = ((0, 1, 2), (1, 2, 0), (2, 0, 1))


def normed(h):
    wide = h.astype(jnp.float32)
    scale = lax.rsqrt(jnp.mean(wide**2, -1, keepdims=True) + 1e-6)
    return (wide * scale).astype(jnp.bfloat16)


def by_normed(h, by_b):
    h, by_b = h.astype(WIDE), by_b.astype(LOW).astype(WIDE)
    scale = lax.rsqrt(jnp.mean(h * h, -1, keepdims=True) + 1e-6)
    return by_b * scale - h * (scale * scale * scale * jnp.mean(by_b * h, -1, keepdims=True))


def angles(tokens):
    half = HEAD // 2
    angle = np.arange(tokens, dtype=np.float32)[:, None] * np.float32(THETA) ** (-np.arange(half, dtype=np.float32) / np.float32(half))
    return jnp.asarray(np.concatenate([np.cos(angle), np.sin(angle)], -1).astype(np.float32))


def _cos_sin(table):
    half = HEAD // 2
    other = pltpu.roll(table, half, 1)
    first = lax.broadcasted_iota(jnp.int32, table.shape, 1) < half
    return jnp.where(first, table, other), jnp.where(first, -other, table)


def _turn(t, cos, sin):
    wide = t.astype(WIDE)
    return (wide * cos + pltpu.roll(wide, HEAD // 2, 1) * sin).astype(LOW)


def _before(h_ref, turn_ref, wq_ref, wk_ref, wv_ref, q_ref, k_ref, v_ref):
    a = normed(h_ref[...])
    cos, sin = _cos_sin(turn_ref[...])
    q = _dot(a, wq_ref[...]).astype(LOW)
    for n in range(q_ref.shape[0]):
        q_ref[n] = _turn(q[:, n * HEAD : (n + 1) * HEAD], cos, sin)
    kv = _dot(a, jnp.concatenate([wk_ref[...], wv_ref[...]], 1)).astype(LOW)
    k_ref[...] = _turn(kv[:, :HEAD], cos, sin)
    v_ref[...] = kv[:, HEAD:]


def _of_layer(number, w):
    return pl.BlockSpec((None, *w.shape[1:]), lambda *_: (number, 0, 0))


def before(number, h, turns, wq, wk, wv, tb=512):
    t, d = h.shape
    heads = wq.shape[2] // HEAD
    row = lambda i: (i, 0)
    return pl.pallas_call(
        _before,
        grid=(t // tb,),
        in_specs=[pl.BlockSpec((tb, d), row), pl.BlockSpec((tb, HEAD), row), *(_of_layer(number, w) for w in (wq, wk, wv))],
        out_specs=[pl.BlockSpec((heads, tb, HEAD), lambda i: (0, i, 0)), pl.BlockSpec((tb, HEAD), row), pl.BlockSpec((tb, HEAD), row)],
        out_shape=[jax.ShapeDtypeStruct((heads, t, HEAD), LOW), jax.ShapeDtypeStruct((t, HEAD), LOW), jax.ShapeDtypeStruct((t, HEAD), LOW)],
        compiler_params=pltpu.CompilerParams(dimension_semantics=("arbitrary",), vmem_limit_bytes=VMEM),
        cost_estimate=pl.CostEstimate(flops=2 * t * d * (heads + 2) * HEAD, transcendentals=t, bytes_accessed=4 * t * d),
        name="before",
    )(h, turns, wq, wk, wv)


def _halve(core, acc_s, refs):
    if len(refs) == 1:
        refs[0][...] = acc_s[...].astype(LOW)
        return
    rows = refs[0].shape[1]
    for n in range(8):
        for to, at in zip(refs, (core, 1 - core)):
            to[n] = acc_s[pl.ds(pl.multiple_of((2 * n + at) * rows, 8), rows), :].astype(LOW)


def _gradient(rows, columns, halves):
    return [jax.ShapeDtypeStruct((8, rows // 16, columns), LOW)] * 2 if halves else [jax.ShapeDtypeStruct((rows, columns), LOW)]


def _at_start(shapes):
    return [pl.BlockSpec(one.shape, lambda i, n=len(one.shape): (0,) * n) for one in shapes]


def _after_back(core_ref, dmid_ref, att_ref, wo_ref, datt_ref, delta_ref, *rest):
    *out_refs, acc_s = rest
    i = pl.program_id(0)
    dmid = dmid_ref[...]
    heads = att_ref.shape[0]
    datt = _dot(dmid, wo_ref[...], cb=1).astype(LOW)
    for n in range(heads):
        one = datt[:, n * HEAD : (n + 1) * HEAD]
        datt_ref[n] = one
        delta_ref[n : n + 1, :] = (one.astype(WIDE) * att_ref[n].astype(WIDE)).T.sum(0, keepdims=True)
    term = jnp.concatenate([_dot(att_ref[n].T, dmid) for n in range(heads)], 0)

    @pl.when(i == 0)
    def _():
        acc_s[...] = term

    @pl.when(i > 0)
    def _():
        acc_s[...] += term

    @pl.when(i == pl.num_programs(0) - 1)
    def _():
        _halve(core_ref[0], acc_s, out_refs)


def after_back(number, core, dmid, att, wo, halves, tb=512):
    t, d = dmid.shape
    heads = att.shape[0]
    head = pl.BlockSpec((heads, tb, HEAD), lambda i: (0, i, 0))
    grad = _gradient(heads * HEAD, d, halves)
    return pl.pallas_call(
        _after_back,
        grid=(t // tb,),
        in_specs=[pl.BlockSpec(memory_space=pltpu.SMEM), pl.BlockSpec((tb, d), lambda i: (i, 0)), head, _of_layer(number, wo)],
        out_specs=[head, pl.BlockSpec((heads, tb), lambda i: (0, i)), *_at_start(grad)],
        out_shape=[jax.ShapeDtypeStruct(att.shape, LOW), jax.ShapeDtypeStruct((heads, t), WIDE), *grad],
        scratch_shapes=[pltpu.VMEM((heads * HEAD, d), WIDE)],
        compiler_params=pltpu.CompilerParams(dimension_semantics=("arbitrary",), vmem_limit_bytes=VMEM),
        cost_estimate=pl.CostEstimate(flops=4 * t * d * heads * HEAD, transcendentals=0, bytes_accessed=8 * t * d),
        name="after_back",
    )(core, dmid, att, wo)


def _before_back(core_ref, h_ref, turn_ref, dq_ref, dk_ref, dv_ref, *rest, inner):
    if inner:
        dmid_ref, wq_ref, wk_ref, wv_ref, dh_ref, *rest = rest
    *out_refs, acc_s = rest
    i = pl.program_id(0)
    cos, sin = _cos_sin(turn_ref[...])
    sin = -sin
    by = jnp.concatenate([_turn(dq_ref[n], cos, sin) for n in range(dq_ref.shape[0])] + [_turn(dk_ref[...], cos, sin), dv_ref[...]], 1)
    term = _dot(normed(h_ref[...]).T, by)

    @pl.when(i == 0)
    def _():
        acc_s[...] = term

    @pl.when(i > 0)
    def _():
        acc_s[...] += term

    if inner:
        w = jnp.concatenate([wq_ref[...], wk_ref[...], wv_ref[...]], 1)
        dh_ref[...] = (dmid_ref[...].astype(WIDE) + by_normed(h_ref[...], _dot(by, w, cb=1))).astype(LOW)

    @pl.when(i == pl.num_programs(0) - 1)
    def _():
        _halve(core_ref[0], acc_s, out_refs)


def before_back(number, core, h, turns, dq, dk, dv, dmid, wq, wk, wv, inner, halves, tb=512):
    t, d = h.shape
    heads = dq.shape[0]
    wide = (heads + 2) * HEAD
    row = lambda i: (i, 0)
    states, head = pl.BlockSpec((tb, d), row), pl.BlockSpec((tb, HEAD), row)
    grad = _gradient(d, wide, halves)
    more = [states, *(_of_layer(number, w) for w in (wq, wk, wv))] if inner else []
    return pl.pallas_call(
        functools.partial(_before_back, inner=inner),
        grid=(t // tb,),
        in_specs=[pl.BlockSpec(memory_space=pltpu.SMEM), states, head, pl.BlockSpec((heads, tb, HEAD), lambda i: (0, i, 0)), head, head, *more],
        out_specs=([states] if inner else []) + _at_start(grad),
        out_shape=([jax.ShapeDtypeStruct((t, d), LOW)] if inner else []) + grad,
        scratch_shapes=[pltpu.VMEM((d, wide), WIDE)],
        compiler_params=pltpu.CompilerParams(dimension_semantics=("arbitrary",), vmem_limit_bytes=VMEM),
        cost_estimate=pl.CostEstimate(flops=4 * t * d * wide if inner else t, transcendentals=t, bytes_accessed=10 * t * d),
        name="before_back",
    )(core, h, turns, dq, dk, dv, *([dmid, wq, wk, wv] if inner else []))


def _mlp_forward(h_ref, att_ref, wo_ref, wg_ref, wu_ref, wd_ref, mid_ref, y_ref, gate_ref, up_ref, b_s, mid_s, acc_s, *, tb, strip):
    j, i = pl.program_id(0), pl.program_id(1)
    last = pl.num_programs(0) - 1
    for at in range(0, tb, strip):
        here = pl.ds(pl.multiple_of(i * tb + at, strip), strip)
        cut = pl.ds(at, strip)

        @pl.when(j == 0)
        def _():
            mid = (h_ref[cut, :].astype(WIDE) + _dot(jnp.concatenate([att_ref[n, cut, :] for n in range(att_ref.shape[0])], 1), wo_ref[...]).astype(LOW).astype(WIDE)).astype(LOW)
            mid_ref[cut, :] = mid
            mid_s[here, :] = mid
            b_s[here, :] = normed(mid)
            acc_s[here, :] = jnp.zeros((strip, acc_s.shape[1]), WIDE)

    here = [pl.ds(pl.multiple_of(i * tb + at, strip), strip) for at in range(0, tb, strip)]
    both = lambda n: [_dot(b_s[here[n], :], w[...]) for w in (wg_ref, wu_ref)]
    ahead = both(0)
    for n in range(len(here)):
        gate, up = ahead
        ahead = both(n + 1) if n + 1 < len(here) else None
        cut = pl.ds(n * strip, strip)
        gate_ref[cut, :] = gate
        up_ref[cut, :] = up
        t = (gate * (0.5 * jnp.tanh(0.5 * gate) + 0.5) * up).astype(LOW)
        acc_s[here[n], :] += _dot(t, wd_ref[...])

    @pl.when(j == last)
    def _():
        here = pl.ds(pl.multiple_of(i * tb, tb), tb)
        y_ref[...] = (mid_s[here, :].astype(WIDE) + acc_s[here, :].astype(LOW).astype(WIDE)).astype(LOW)


def _of_mlp(number, d, fb):
    side = pl.BlockSpec((None, d, fb), lambda j, i: (number, 0, j))
    return side, side, pl.BlockSpec((None, fb, d), lambda j, i: (number, j, 0))


def mlp_forward(number, h, att, wo, wg, wu, wd, tb=1024, fb=1024, strip=512):
    t, d = h.shape
    ff, hd = wg.shape[2], wo.shape[1]
    n = t // tb
    at_first = lambda j, i: (jnp.where(j == 0, i, n - 1), 0)
    at_last = lambda j, i: (jnp.where(j == ff // fb - 1, i, 0), 0)
    return pl.pallas_call(
        functools.partial(_mlp_forward, tb=tb, strip=strip),
        grid=(ff // fb, n),
        in_specs=[pl.BlockSpec((tb, d), at_first), pl.BlockSpec((att.shape[0], tb, HEAD), lambda j, i: (0, at_first(j, i)[0], 0)), _of_layer(number, wo),
                  *_of_mlp(number, d, fb)],
        out_specs=[pl.BlockSpec((tb, d), at_first), pl.BlockSpec((tb, d), at_last),
                   *[pl.BlockSpec((tb, fb), lambda j, i: (i, j))] * 2],
        scratch_shapes=[pltpu.VMEM((t, d), LOW), pltpu.VMEM((t, d), LOW), pltpu.VMEM((t, d), WIDE)],
        out_shape=[jax.ShapeDtypeStruct((t, d), LOW), jax.ShapeDtypeStruct((t, d), LOW), jax.ShapeDtypeStruct((t, ff), WIDE),
                   jax.ShapeDtypeStruct((t, ff), WIDE)],
        compiler_params=pltpu.CompilerParams(dimension_semantics=("arbitrary", "arbitrary"), vmem_limit_bytes=VMEM),
        cost_estimate=pl.CostEstimate(flops=2 * t * d * (3 * ff + hd), transcendentals=t * ff, bytes_accessed=8 * t * ff + 6 * d * ff + 10 * t * d),
        name="mlp_forward",
    )(h, att, wo, wg, wu, wd)


def _mlp_backward(core_ref, dy_ref, mid_ref, gate_ref, up_ref, wg_ref, wu_ref, wd_ref, dmid_ref, *rest, tb, strip):
    *out_refs, bt_s, dyt_s, db_s, pg_s, pu_s, t_s, ag_s, au_s, ad_s = rest
    per = len(out_refs) // 3
    j, i = pl.program_id(0), pl.program_id(1)
    all_i = pl.ds(pl.multiple_of(i * tb, tb), tb)

    @pl.when(j == 0)
    def _():
        for at in range(0, tb, strip):
            here = pl.ds(pl.multiple_of(i * tb + at, strip), strip)
            bt_s[:, here] = normed(mid_ref[here, :]).T
            dyt_s[:, here] = dy_ref[here, :].T
            db_s[here, :] = jnp.zeros((strip, db_s.shape[1]), WIDE)

    @pl.when(i == 0)
    def _():
        for ref in (ag_s, au_s, ad_s):
            ref[...] = jnp.zeros_like(ref)

    for at in range(0, tb, strip):
        here = pl.ds(pl.multiple_of(i * tb + at, strip), strip)
        cut = pl.ds(at, strip)
        dt = _dot(dy_ref[here, :], wd_ref[...], cb=1).astype(LOW).astype(WIDE)
        gate, up = gate_ref[cut, :], up_ref[cut, :]
        half = 0.5 * jnp.tanh(0.5 * gate)
        sig = half + 0.5
        silu = gate * sig
        by_up = (dt * silu).astype(LOW)
        by_gate = (dt * up * (sig + silu * (0.5 - half))).astype(LOW)
        t_s[cut, :] = (silu * up).astype(LOW)
        pg_s[cut, :] = by_gate
        pu_s[cut, :] = by_up
        db_s[here, :] += _dot(by_gate, wg_ref[...], cb=1) + _dot(by_up, wu_ref[...], cb=1)

    ag_s[...] += _dot(bt_s[:, all_i], pg_s[...])
    au_s[...] += _dot(bt_s[:, all_i], pu_s[...])
    ad_s[...] += _dot(dyt_s[:, all_i], t_s[...])

    @pl.when(i == pl.num_programs(1) - 1)
    def _():
        core = core_ref[0]
        _halve(core, ag_s, out_refs[:per])
        _halve(core, au_s, out_refs[per : 2 * per])
        down = out_refs[2 * per :]
        if per == 1:
            down[0][...] = ad_s[...].T.astype(LOW)
        else:
            wide = down[0].shape[1]
            for to, at in zip(down, (core, 1 - core)):
                to[0] = ad_s[:, pl.ds(pl.multiple_of(at * wide, 128), wide)].T.astype(LOW)

    @pl.when(j == pl.num_programs(0) - 1)
    def _():
        for at in range(0, tb, strip):
            here = pl.ds(pl.multiple_of(i * tb + at, strip), strip)
            cut = pl.ds(at, strip)
            dmid_ref[cut, :] = (dy_ref[here, :].astype(WIDE) + by_normed(mid_ref[here, :], db_s[here, :])).astype(LOW)


def mlp_backward(number, core, dy, mid, gate, up, wg, wu, wd, halves, tb=1024, strip=256):
    t, d = dy.shape
    ff = wg.shape[2]
    n, fb = t // tb, ff // 8
    whole = lambda j, i: (0, 0)
    at_last = lambda j, i: (jnp.where(j == 7, i, 0), 0)
    rows = d // 16
    if halves:
        side, tall = [pl.BlockSpec((8, rows, fb), lambda j, i: (0, 0, j))] * 2, [pl.BlockSpec((1, fb // 2, d), lambda j, i: (j, 0, 0))] * 2
    else:
        side, tall = [pl.BlockSpec((d, fb), lambda j, i: (0, j))], [pl.BlockSpec((fb, d), lambda j, i: (j, 0))]
    one = pl.Buffered(1)
    return pl.pallas_call(
        functools.partial(_mlp_backward, tb=tb, strip=strip),
        grid=(8, n),
        in_specs=[pl.BlockSpec(memory_space=pltpu.SMEM), pl.BlockSpec((t, d), whole, pipeline_mode=one), pl.BlockSpec((t, d), whole, pipeline_mode=one),
                  *[pl.BlockSpec((tb, fb), lambda j, i: (i, j))] * 2,
                  *_of_mlp(number, d, fb)],
        out_specs=[pl.BlockSpec((tb, d), at_last), *side, *side, *tall],
        scratch_shapes=[pltpu.VMEM((d, t), LOW), pltpu.VMEM((d, t), LOW), pltpu.VMEM((t, d), WIDE)] + [pltpu.VMEM((tb, fb), LOW)] * 3
        + [pltpu.VMEM((d, fb), WIDE)] * 3,
        out_shape=[jax.ShapeDtypeStruct((t, d), LOW), *_gradient(d, ff, halves), *_gradient(d, ff, halves), *_gradient(ff, d, halves)],
        compiler_params=pltpu.CompilerParams(dimension_semantics=("arbitrary", "arbitrary"), vmem_limit_bytes=VMEM),
        cost_estimate=pl.CostEstimate(flops=12 * t * d * ff, transcendentals=t * ff, bytes_accessed=8 * t * ff + 12 * d * ff + 6 * t * d),
        name="mlp_backward",
    )(core, dy, mid, gate, up, wg, wu, wd)


def swapped(t, step):
    return lax.ppermute(t, "dp", [(n, n ^ step) for n in range(16)])


class Reduction:
    def __init__(self, place, pairs, orders):
        self.place, self.orders, self.at = place, orders, 0
        self.held = [[keep.reshape(2, 2, 2, *keep.shape[1:])] for keep, _ in pairs]
        self.out = [send for _, send in pairs]

    def go(self):
        self.got = [swapped(t, AXES[order[self.at - 1]] if self.at else 1) for t, order in zip(self.out, self.orders)]

    def take(self):
        total = lambda parts: functools.reduce(jnp.add, [p.astype(WIDE) for p in parts]).astype(LOW)
        for n, order in enumerate(self.orders[: len(self.out)]):
            self.held[n].append(self.got[n].reshape(self.held[n][0].shape))
            if self.at == 3:
                self.out[n] = total(self.held[n]).reshape(self.held[n][0].shape[3:])
                continue
            axis = order[self.at]
            mine = self.place // AXES[axis] % 2
            pick = lambda t, at: lax.dynamic_index_in_dim(t, at, axis, keepdims=True)
            self.out[n] = total([pick(t, 1 - mine) for t in self.held[n]])
            self.held[n] = [pick(t, mine) for t in self.held[n]]
        self.at += 1


def landed(x, *reductions):
    x, got = lax.optimization_barrier((x, [r.got for r in reductions]))
    for r, new in zip(reductions, got):
        r.got = new
        r.take()
    x, out = lax.optimization_barrier((x, [r.out for r in reductions]))
    for r, new in zip(reductions, out):
        r.out = new
        if r.at < 4:
            r.go()
    return x


MESH_ID = pl.DeviceIdType.MESH


def _squares(*refs):
    *in_refs, o_ref, own_s, all_s, send_sem, recv_sem = refs
    me = lax.axis_index("dp")
    barrier = pltpu.get_barrier_semaphore()
    for n in range(1, 16):
        pl.semaphore_signal(barrier, inc=1, device_id={"dp": (me + n) % 16}, device_id_type=MESH_ID)
    total = jnp.zeros(own_s.shape, WIDE)
    for ref in in_refs:
        x = ref[...].astype(WIDE)
        x = (x * x).reshape(-1, 8, x.shape[1]).sum(0)
        for at in range(0, x.shape[1], 128):
            total += x[:, at : at + 128]
    own_s[...] = total
    pl.semaphore_wait(barrier, 15)
    copies = [pltpu.make_async_remote_copy(src_ref=own_s, dst_ref=all_s.at[n], send_sem=send_sem.at[n], recv_sem=recv_sem.at[n],
                                           device_id={"dp": (me + n) % 16}, device_id_type=MESH_ID) for n in range(1, 16)]
    for copy in copies:
        copy.start()
    for copy in copies:
        copy.wait()
    for n in range(1, 16):
        total += all_s[n]
    o_ref[...] = jnp.broadcast_to(jnp.sum(total, keepdims=True), o_ref.shape)


def squares(arrays):
    vmem = pl.BlockSpec(memory_space=pltpu.VMEM)
    tile = (8, 128)
    return pl.pallas_call(
        _squares,
        in_specs=[vmem] * len(arrays),
        out_specs=vmem,
        out_shape=jax.ShapeDtypeStruct(tile, WIDE),
        scratch_shapes=[pltpu.VMEM(tile, WIDE), pltpu.VMEM((16, *tile), WIDE), pltpu.SemaphoreType.DMA((16,)), pltpu.SemaphoreType.DMA((16,))],
        compiler_params=pltpu.CompilerParams(collective_id=0, has_side_effects=True),
        name="squares",
    )(*arrays)


def _gathered(*refs, turns):
    n = len(turns)
    ins, outs = refs[:n], refs[n : 2 * n]
    ici_send, ici_recv, pair_send, pair_recv, own_sem = refs[2 * n :]
    me = lax.axis_index("dp")
    steps = [s * (1 - 2 * (me // s % 2)) for s in AXES]
    other = 1 - 2 * (me % 2)
    barrier = pltpu.get_barrier_semaphore()
    for step in (*steps, other):
        pl.semaphore_signal(barrier, inc=1, device_id={"dp": me + step}, device_id_type=MESH_ID)
    pl.semaphore_wait(barrier, 4)

    def block(mask):
        return me + sum(steps[a] for a in range(3) if mask >> a & 1)

    def copy(k, mask, to, sems, row):
        src = ins[k] if mask == 0 else outs[k].at[:, block(mask)]
        return pltpu.make_async_remote_copy(src_ref=src, dst_ref=outs[k].at[:, block(mask)], send_sem=sems[0].at[k, row], recv_sem=sems[1].at[k, row],
                                            device_id={"dp": me + to}, device_id_type=MESH_ID)

    started = []

    def go(k, mask):
        order = ORDERS[turns[k]]
        last = max([order.index(a) for a in range(3) if mask >> a & 1], default=-1)
        for a in order[last + 1 :]:
            one = copy(k, mask, steps[a], (ici_send, ici_recv), mask | 1 << a)
            one.start()
            started.append(one)
        one = copy(k, mask, other, (pair_send, pair_recv), mask)
        one.start()
        started.append(one)

    def here(k, mask):
        copy(k, mask, steps[0], (ici_send, ici_recv), mask).wait_recv()
        go(k, mask)

    mine = [pltpu.make_async_copy(ins[k], outs[k].at[:, me], own_sem.at[k]) for k in range(n)]
    for k in range(n):
        go(k, 0)
    for one in mine:
        one.start()
    bit = lambda k, *at: sum(1 << ORDERS[turns[k]][a] for a in at)
    for sets in (((0,), (1,), (2,)), ((0, 1), (0, 2), (1, 2)), ((0, 1, 2),)):
        for k in range(n):
            for at in sets:
                here(k, bit(k, *at))
    for k in range(n):
        for mask in range(8):
            copy(k, mask, other, (pair_send, pair_recv), mask).wait_recv()
    for one in started:
        one.wait_send()
    for one in mine:
        one.wait()


def gathered(blocks, turns):
    hbm = pl.BlockSpec(memory_space=pl.ANY)
    n = len(blocks)
    sems = [pltpu.SemaphoreType.DMA((n, 8))] * 4 + [pltpu.SemaphoreType.DMA((n,))]
    return pl.pallas_call(
        functools.partial(_gathered, turns=turns),
        in_specs=[hbm] * n,
        out_specs=[hbm] * n,
        out_shape=[jax.ShapeDtypeStruct((b.shape[0], 16, *b.shape[1:]), b.dtype) for b in blocks],
        scratch_shapes=sems,
        compiler_params=pltpu.CompilerParams(collective_id=1, has_side_effects=True, vmem_limit_bytes=2**20),
        name="gathered",
    )(*blocks)


def _settled(*refs):
    n = len(refs) // 2
    copies = [pltpu.make_async_copy(refs[k], refs[n + k], refs[-1].at[k]) for k in range(n)]
    for copy in copies:
        copy.start()
    for copy in copies:
        copy.wait()


def settled(arrays):
    hbm = pl.BlockSpec(memory_space=pl.ANY)
    n = len(arrays)
    return pl.pallas_call(
        _settled,
        in_specs=[hbm] * n,
        out_specs=[hbm] * n,
        out_shape=[jax.ShapeDtypeStruct(a.shape, a.dtype) for a in arrays],
        scratch_shapes=[pltpu.SemaphoreType.DMA((n,))],
        compiler_params=pltpu.CompilerParams(vmem_limit_bytes=2**20),
        name="settled",
    )(*arrays)


def adamw(w, m, v, g):
    m = 0.9 * m + 0.1 * g
    v = 0.95 * v + 0.05 * g * g
    step = m * lax.rsqrt(v + 1e-8) + 0.1 * w
    return (w - 0.02 * step).astype(jnp.bfloat16), m, v


def clipped(gradients, sum_of_squares, count):
    factor = jnp.minimum(1.0, 0.5 * lax.rsqrt(sum_of_squares / count + 1e-30))
    return [g * factor for g in gradients]


def solution(mesh):
    def step(x, dy, *arrays):
        weights, m, v = (arrays[i : i + 7] for i in (0, 7, 14))
        layers = weights[0].shape[0]
        me = lax.axis_index("dp")
        core = (me % 2).astype(jnp.int32).reshape(1)
        wq, wk, wv, wo, wg, wu, wd = weights
        turns = angles(x.shape[1])
        h, kept = x[0], []
        for number in range(layers):
            q, k, val = before(number, h, turns, wq, wk, wv)
            att, lse = attend(q, k, val)
            mid, y, gate, up = mlp_forward(number, h, att, wo, wg, wu, wd)
            kept.append((h, q, k, val, att, lse, mid, gate, up))
            h = y
        by_h = dy[0]
        scattered = lambda t: lax.psum_scatter(t, "dp", scatter_dimension=0, tiled=True)
        dq, dk = wq.shape[2], wk.shape[2]
        late_mlp, late_small = [], []
        for number in reversed(range(layers)):
            h, q, k, val, att, lse, mid, gate, up = kept[number]
            last = number == 0
            by_mid, *by_mlp = mlp_backward(number, core, by_h, mid, gate, up, wg, wu, wd, last)
            if last:
                big = Reduction(me, [by_mlp[n : n + 2] for n in (0, 2, 4)], ORDERS)
                big.go()
                by_mid, late_small, sides = lax.optimization_barrier((by_mid, late_small, [m[:2] for m in late_mlp]))
                late_small = [scattered(some) for some in late_small]
            by_att, delta, *by_o = after_back(number, core, by_mid, att, wo, last)
            if last:
                by_att = landed(by_att, big)
                out = Reduction(me, [by_o], ORDERS[1:])
                out.go()
            by_q, by_k, by_v = attend_back(q, k, val, by_att, lse, delta)
            if last:
                by_q = landed(by_q, out)
            outs = before_back(number, core, h, turns, by_q, by_k, by_v, by_mid, wq, wk, wv, not last, last)
            if not last:
                by_h, by_qkv = outs
                late_mlp.append([scattered(t) for t in by_mlp])
                by_o = by_o[0].reshape(16, -1, by_o[0].shape[1])
                by_qkv = by_qkv.reshape(16, -1, by_qkv.shape[1])
                wider = ((0, 0), (0, 0), (0, by_qkv.shape[2] - by_o.shape[2]))
                late_small.append(jnp.concatenate([by_qkv, jnp.pad(by_o, wider)], 1).reshape(-1, by_qkv.shape[2]))
        outs, downs = lax.optimization_barrier((landed(outs, big), [m[2] for m in late_mlp]))
        small = Reduction(me, [outs], ORDERS)
        small.go()
        for r in (big, small, out):
            while r.at < 4:
                r.take()
                if r.at < 4:
                    r.go()
        rows = wq.shape[1] // 16
        mine = [[*small.out, *out.out, *big.out]]
        mine += [[some[:rows], some[rows:, : wo.shape[2]], *side, down] for some, side, down in zip(late_small, sides, downs)][::-1]
        total = squares([t for some in mine for t in some])[0, 0]
        mine = [[qkv[:, :dq], qkv[:, dq : dq + dk], qkv[:, dq + dk :], *rest] for qkv, *rest in mine]
        gradients = [jnp.stack([some[i] for some in mine]).astype(WIDE) for i in range(7)]
        gradients = clipped(gradients, total, 16 * sum(g.size for g in gradients))
        own = [lax.dynamic_slice_in_dim(w, me * one.shape[1], one.shape[1], 1).astype(jnp.float32) for w, one in zip(weights, m, strict=True)]
        new = [adamw(w, m, v, g) for w, m, v, g in zip(own, m, v, gradients, strict=True)]
        whole = gathered([one[0] for one in new], (0, 1, 1, 2, 0, 1, 2))
        whole = [t.reshape(t.shape[0], -1, t.shape[3]) for t in settled(whole)]
        return (*whole, *(one[1] for one in new), *(one[2] for one in new))

    states, all_of, cut = P(("rep", "dp"), None, None), P(None, None, None), P(None, "dp", None)
    return jax.shard_map(
        step,
        mesh=mesh,
        in_specs=(states, states) + (all_of,) * 7 + (cut,) * 14,
        out_specs=(P("rep", None, None),) * 7 + (P("rep", "dp", None),) * 14,
        check_vma=False,
    )
```
